128 devices in a mesh: dap: 32 (over z, x, y_lo), head: 4 (over y_hi, core).
Axes of the slice: x: 4, y: 4 (y_hi: 2, y_lo: 2; y = y_hi * 2 + y_lo), z: 4, core: 2. Of those that a mesh axis runs over, the one named last changes fastest.
Arguments:
- multiple_aligned_family: bfloat16 [512, 512, 256], P('dap')
- homolog_present_flags: int32 [512], replicated, may hold values from 0 to 1, as said below
- amino_present_flags: int32 [512], replicated, may hold values 0 or 1
- focus_layernorm_scaling: float32 [256], replicated, may hold values from 0.5 to 1.5
- focus_layernorm_offset: float32 [256], replicated, may hold values from -1.8 to 1.8
- combined_focus_matrices: bfloat16 [256, 4, 256], P(None, None, 'head')
- sigmoid_switch_offset: float32 [256], P('head'), may hold values from -4 to 4
- focus_final_matrix: bfloat16 [256, 256], P('head'), may hold values from -0.375 to 0.375
- focus_final_offset: float32 [256], replicated, may hold values from -3 to 3
- tensor_layernorm_scaling: float32 [256], replicated, may hold values from 0.5 to 1.5
- tensor_layernorm_offset: float32 [256], replicated, may hold values from -1.8 to 1.8
- tensor_product_factors: bfloat16 [256, 2, 32], replicated, may hold values from -0.375 to 0.375
- tensor_final_matrix: float32 [1024, 128], replicated, may hold values from -0.1875 to 0.1875
- tensor_final_offset: float32 [128], replicated, may hold values from -4 to 4
Outputs:
- alignment_output: bfloat16 [512, 512, 256], P(('dap', 'head'))
- pair_mean_update: float32 [512, 512, 128], P('dap', 'head')
The draws below stay inside these ranges and needn't reach their ends.
Inputs may be any that keep to these rules, and one draw needn't show every extreme that they name: homolog_present_flags[0] is always 1.
All inputs are finite; a program needn't handle non-finite values.
Results may differ from the reference program's by a relative error of at most 0.005.
Values may be sent and summed in bfloat16 or wider, within the bound.
No kernel may reach another device: no remote copies, remote signals or barrier semaphores. Data moves between devices by JAX's collectives and lax.ppermute only.
A program may use at most 256 MiB of HBM per device.

```python
import math
import jax
import jax.numpy as jnp
from jax import lax

C = 256
H = 8
DH = 32
CZ = 128
CO = 32
RES_DEV = 16
S = 512
R = 512


def draw_multiple_aligned_family(key, part):
    keys = jax.random.split(jax.random.fold_in(key, 11), 3)
    profile = jax.random.normal(keys[0], (R, C), jnp.float32)
    noise = jax.random.normal(keys[1], (S, R, C), jnp.float32)
    seq_scale = jnp.exp(jax.random.uniform(keys[2], (S, 1, 1), jnp.float32, math.log(0.5), math.log(2.0)))
    mixed = profile[None] + noise * seq_scale
    return jnp.clip(mixed, -12.0, 12.0).astype(jnp.bfloat16)


def draw_combined_focus_matrices(key, part):
    keys = jax.random.split(jax.random.fold_in(key, 23), 1)
    weights = jax.random.normal(keys[0], (C, 4, H * DH), jnp.float32) * C ** (-0.5)
    return weights.astype(jnp.bfloat16)


def draw_homolog_present_flags(key, part):
    picks = jax.random.randint(jax.random.fold_in(key, 37), (S,), 0, 4)
    present = (picks > 0).astype(jnp.int32)
    return present.at[0].set(1)


def place_ends(values, rng, smallest, top_value):
    index_at = [jax.random.randint(jax.random.fold_in(rng, axis), (), 0, length) for axis, length in enumerate(values.shape)]
    main_axis = values.shape.index(max(values.shape))
    beside = index_at[:main_axis] + [(index_at[main_axis] + 1) % values.shape[main_axis]] + index_at[main_axis + 1:]
    return values.at[tuple(index_at)].set(smallest).at[tuple(beside)].set(top_value)


def block_scale(own_key, shape, cuts, low, top_value):
    level, own = 1.0, jax.random.fold_in(own_key, 6)
    for axis_at, blocks in cuts:
        heights = jnp.exp(jax.random.uniform(jax.random.fold_in(own, axis_at), (blocks,), jnp.float32, low / len(cuts), top_value / len(cuts)))
        level = level * jnp.repeat(heights, shape[axis_at] // blocks).reshape([-1 if axis == axis_at else 1 for axis in range(len(shape))])
    return level


def bell_draw(stream_key, extent, width, most, cuts=(), dtype=jnp.bfloat16):
    array = width * jax.random.normal(stream_key, extent, jnp.float32)
    if cuts:
        array = array * block_scale(stream_key, extent, cuts, -0.22, 0.18)
    return jnp.clip(array, -most, most).astype(dtype)


def setup_inputs(seed: int = 0) -> dict:
    streams_of = jax.random.split(jax.random.key(seed), 15)
    multiple_aligned_family = draw_multiple_aligned_family(jax.random.fold_in(streams_of[14], 71), 0)
    homolog_present_flags = draw_homolog_present_flags(jax.random.fold_in(streams_of[14], 71), 0)
    amino_present_flags = place_ends((jax.random.randint(streams_of[2], (R,), 0, 8) < 7).astype(jnp.int32), jax.random.fold_in(streams_of[2], 1), 0, 1)
    focus_layernorm_scaling = jnp.clip(1.0 + 0.1 * jax.random.normal(streams_of[3], (C,), jnp.float32), 0.5, 1.5)
    focus_layernorm_offset = bell_draw(streams_of[4], (C,), 0.3, 1.8, (), jnp.float32)
    combined_focus_matrices = draw_combined_focus_matrices(jax.random.fold_in(streams_of[14], 71), 0)
    sigmoid_switch_offset = bell_draw(streams_of[6], (H * DH,), 1.0, 4.0, ((0, 4),), jnp.float32)
    focus_final_matrix = bell_draw(streams_of[7], (H * DH, C), (H * DH) ** -0.5, 0.375, ((0, 4),))
    focus_final_offset = bell_draw(streams_of[8], (C,), 0.5, 3.0, (), jnp.float32)
    tensor_layernorm_scaling = jnp.clip(1.0 + 0.1 * jax.random.normal(streams_of[9], (C,), jnp.float32), 0.5, 1.5)
    tensor_layernorm_offset = bell_draw(streams_of[10], (C,), 0.3, 1.8, (), jnp.float32)
    tensor_product_factors = bell_draw(streams_of[11], (C, 2, CO), C ** -0.5, 0.375)
    tensor_final_matrix = bell_draw(streams_of[12], (CO * CO, CZ), (CO * CO) ** -0.5, 0.1875, (), jnp.float32)
    tensor_final_offset = bell_draw(streams_of[13], (CZ,), 1.0, 4.0, (), jnp.float32)
    return {"multiple_aligned_family": multiple_aligned_family, "homolog_present_flags": homolog_present_flags, "amino_present_flags": amino_present_flags, "focus_layernorm_scaling": focus_layernorm_scaling, "focus_layernorm_offset": focus_layernorm_offset, "combined_focus_matrices": combined_focus_matrices, "sigmoid_switch_offset": sigmoid_switch_offset, "focus_final_matrix": focus_final_matrix, "focus_final_offset": focus_final_offset, "tensor_layernorm_scaling": tensor_layernorm_scaling, "tensor_layernorm_offset": tensor_layernorm_offset, "tensor_product_factors": tensor_product_factors, "tensor_final_matrix": tensor_final_matrix, "tensor_final_offset": tensor_final_offset}


def layer_norm(value, gain, bias):
    mean = lax.optimization_barrier(jnp.mean(value, -1, keepdims=True))
    centred = value - mean
    spread = lax.optimization_barrier(jnp.mean(centred * centred, -1, keepdims=True))
    return centred * lax.rsqrt(spread + 1e-05) * gain + bias

def reference(multiple_aligned_family, homolog_present_flags, amino_present_flags, focus_layernorm_scaling, focus_layernorm_offset, combined_focus_matrices, sigmoid_switch_offset, focus_final_matrix, focus_final_offset, tensor_layernorm_scaling, tensor_layernorm_offset, tensor_product_factors, tensor_final_matrix, tensor_final_offset):
    keep = homolog_present_flags > 0
    weights_in = combined_focus_matrices.reshape(C, 4 * H * DH)
    gate_shift = sigmoid_switch_offset.reshape(H, DH)

    def lengthwise_portion(column_rows):
        normed = layer_norm(column_rows.astype(jnp.float32), focus_layernorm_scaling, focus_layernorm_offset).astype(jnp.bfloat16)
        projected = jnp.dot(normed, weights_in, preferred_element_type=jnp.float32).reshape(S, 4, H, DH)
        query = (projected[:, 0] * DH ** (-0.5)).astype(jnp.bfloat16)
        keys = projected[:, 1].astype(jnp.bfloat16)
        values = projected[:, 2].astype(jnp.bfloat16)
        gate = jax.nn.sigmoid(projected[:, 3] + gate_shift)
        scores = jnp.einsum('shd,thd->hst', query.astype(jnp.float32), keys.astype(jnp.float32))
        scores = jnp.where(keep[None, None, :], scores, jnp.float32(-1000000000.0))
        top = lax.optimization_barrier(jnp.max(scores, -1, keepdims=True))
        weights = jnp.exp(scores - top)
        probs = (weights / lax.optimization_barrier(jnp.sum(weights, -1, keepdims=True))).astype(jnp.bfloat16)
        mixed = jnp.einsum('hst,thd->shd', probs.astype(jnp.float32), values.astype(jnp.float32))
        attended = (mixed * gate).astype(jnp.bfloat16).reshape(S, H * DH)
        update = jnp.dot(attended, focus_final_matrix, preferred_element_type=jnp.float32)
        return (column_rows.astype(jnp.float32) + update + focus_final_offset).astype(jnp.bfloat16)
    refreshed_embedding = lax.map(lengthwise_portion, jnp.moveaxis(multiple_aligned_family, 1, 0))
    alignment_output = jnp.moveaxis(refreshed_embedding, 0, 1)
    opm_normed = layer_norm(refreshed_embedding.astype(jnp.float32), tensor_layernorm_scaling, tensor_layernorm_offset).astype(jnp.bfloat16)
    both = jnp.dot(opm_normed.reshape(R * S, C), tensor_product_factors.reshape(C, 2 * CO), preferred_element_type=jnp.float32).reshape(R, S, 2, CO)
    keep_rs = amino_present_flags.astype(jnp.float32)[:, None] * homolog_present_flags.astype(jnp.float32)[None, :]
    left = (both[:, :, 0] * keep_rs[:, :, None]).astype(jnp.bfloat16)
    right = (both[:, :, 1] * keep_rs[:, :, None]).astype(jnp.bfloat16)
    right_wide = right.astype(jnp.float32)

    def rows(left_block):
        outer = jnp.einsum('isc,jse->ijce', left_block.astype(jnp.float32), right_wide)
        flat = outer.reshape(RES_DEV * R, CO * CO)
        return jnp.dot(flat, tensor_final_matrix, precision=lax.Precision.HIGHEST, preferred_element_type=jnp.float32).reshape(RES_DEV, R, CZ)
    projected_pair = lax.map(rows, left.reshape(R // RES_DEV, RES_DEV, S, CO)).reshape(R, R, CZ)
    count = jnp.sum(homolog_present_flags).astype(jnp.float32)
    res_keep = amino_present_flags.astype(jnp.float32)
    norm = jnp.maximum(count * res_keep[:, None] * res_keep[None, :], 1.0)
    pair_mean_update = (projected_pair + tensor_final_offset) / norm[:, :, None]
    return (alignment_output, pair_mean_update)
```

```python
import math

import jax
import jax.numpy as jnp
from jax import lax
from jax.experimental import pallas as pl
from jax.experimental.pallas import tpu as pltpu
from jax.sharding import PartitionSpec as P

DH = 32
CO = 32
LOG2E = math.log2(math.e)
NT = (((1,), (1,)), ((), ()))
TN = (((0,), (0,)), ((), ()))
F32 = jnp.float32
BF16 = jnp.bfloat16


def layer_norm(value, gain, bias):
    mean = jnp.mean(value, -1, keepdims=True)
    centred = value - mean
    spread = jnp.mean(centred * centred, -1, keepdims=True)
    return centred * lax.rsqrt(spread + 1e-05) * gain + bias


def attend_kernel(
    amino_ref,
    x_ref,
    w_ref,
    shift_ref,
    gain_ref,
    bias_ref,
    out_bias_ref,
    gain2_ref,
    bias2_ref,
    keep_col_ref,
    keep_row_ref,
    right_weight_ref,
    left_weight_ref,
    rows_ref,
    left_ref,
    right_ref,
    q_ref,
    k_ref,
    v_ref,
    g_ref,
    a_ref,
    rows_scratch,
    right_scratch,
):
    step = pl.program_id(0)
    steps = pl.num_programs(0)
    groups, unit, chans = w_ref.shape
    width = chans // groups
    seqs = keep_col_ref.shape[0]
    x = x_ref[...].reshape(seqs, chans).astype(F32)
    normed = layer_norm(x, gain_ref[...], bias_ref[...]).astype(BF16)

    def weight(which):
        return w_ref[:, which * width : (which + 1) * width, :].reshape(groups * width, chans)

    def transposed(which):
        return lax.dot_general(weight(which), normed, NT, preferred_element_type=F32)

    q_ref[...] = (transposed(0) * (DH**-0.5 * LOG2E)).astype(BF16)
    k_ref[...] = lax.dot_general(normed, weight(1), NT, preferred_element_type=F32).astype(BF16)
    v_ref[...] = transposed(2).astype(BF16)
    g_ref[...] = jax.nn.sigmoid(transposed(3) + shift_ref[...])
    present = jnp.broadcast_to(keep_col_ref[...], (seqs, seqs)) > 0.0
    ones = jnp.ones((16, seqs), BF16)
    for head in range(chans // DH):
        low, high = head * DH, (head + 1) * DH
        scores = jnp.dot(k_ref[:, low:high], q_ref[low:high, :], preferred_element_type=F32)
        scores = jnp.where(present, scores, F32(-1e9 * LOG2E))
        top = jnp.max(scores, 0, keepdims=True)
        probs = jnp.exp2(scores - top).astype(BF16)
        both = jnp.concatenate([v_ref[low:high, :], ones], 0)
        mixed = jnp.dot(both, probs, preferred_element_type=F32)
        scale = 1.0 / mixed[DH : DH + 1, :]
        a_ref[low:high, :] = (mixed[:DH, :] * scale * g_ref[low:high, :]).astype(BF16)
    update = lax.dot_general(a_ref[...], weight(4), TN, preferred_element_type=F32)
    fresh = (x + update + out_bias_ref[...]).astype(BF16)
    wide = fresh.astype(F32)
    for part in range(chans // 128):
        rows_scratch[part, pl.ds(step, seqs, stride=steps), :] = wide[:, part * 128 : (part + 1) * 128]
    opm = layer_norm(wide, gain2_ref[...], bias2_ref[...]).astype(BF16)
    here = amino_ref[step].astype(F32)
    left = lax.dot_general(left_weight_ref[...], opm, NT, preferred_element_type=F32)
    left_ref[...] = (left * (keep_row_ref[...] * here)).astype(BF16)[None]
    right = jnp.dot(opm, right_weight_ref[...], preferred_element_type=F32)
    right = right * (keep_col_ref[...] * here)

    @pl.when(step == 0)
    def _():
        right_scratch[...] = right

    @pl.when(step > 0)
    def _():
        right_scratch[...] += right

    @pl.when(step == steps - 1)
    def _():
        right_ref[...] = right_scratch[...].astype(BF16)
        for part in range(chans // 128):
            rows_ref[:, part * 128 : (part + 1) * 128] = rows_scratch[part].astype(BF16)


def pair_kernel(left_ref, right_ref, weight_ref, bias_ref, inverse_ref, out_ref, mid_ref):
    step = pl.program_id(0)
    count, seqs, lanes = right_ref.shape
    rows = out_ref.shape[0]
    pieces = jnp.concatenate([right_ref[q] for q in range(count)], 1)
    outer = jnp.dot(left_ref[...], pieces, preferred_element_type=F32).astype(BF16)
    for q in range(count):
        at = pl.multiple_of((step * count + q) * rows, rows)
        for c in range(CO):
            mid_ref[pl.ds(at, rows), c * lanes : (c + 1) * lanes] = outer[
                c * rows : (c + 1) * rows, q * lanes : (q + 1) * lanes
            ]

    @pl.when(step == pl.num_programs(0) - 1)
    def _():
        total = jnp.dot(mid_ref[...], weight_ref[...], preferred_element_type=F32)
        depth = bias_ref.shape[1]
        blocks = total.shape[0] // rows
        inner = lanes // CO
        for k in range(inner):
            part = (total[:, k * depth : (k + 1) * depth] + bias_ref[...]) * inverse_ref[
                :, k : k + 1
            ]
            for b in range(blocks):
                out_ref[:, b * inner + k, :] = part[b * rows : (b + 1) * rows]


def whole(shape):
    return pl.BlockSpec(shape, lambda *_: (0,) * len(shape))


def per_device(
    msa,
    homolog,
    amino,
    gain,
    bias,
    focus,
    switch,
    final,
    final_bias,
    gain2,
    bias2,
    factors,
    pair_weight,
    pair_bias,
):
    n_dap, n_head = lax.axis_size("dap"), lax.axis_size("head")
    head_id, dap_id = lax.axis_index("head"), lax.axis_index("dap")
    own_seqs, residues, chans = msa.shape
    seqs = homolog.shape[0]
    width = focus.shape[2]
    col_width = residues // n_head
    mine = col_width // n_dap
    nz, nx, ny = 4, 4, 2

    parts = jnp.moveaxis(focus, 0, 2).reshape(4 * width, chans)
    first = lax.reduce_precision(switch, 8, 7)
    second = lax.reduce_precision(switch - first, 8, 7)
    third = switch - first - second
    offsets = jnp.zeros((16, chans), BF16)
    offsets = offsets.at[:3, :width].set(jnp.stack([first, second, third]).astype(BF16))
    bundle = jnp.concatenate([parts, final, offsets], 0)
    weights = lax.all_gather(bundle, "head", axis=0, tiled=False)
    base = 5 * width
    shift = weights[:, base : base + 3, :width].astype(F32)
    shift = ((shift[:, 0] + shift[:, 1]) + shift[:, 2]).reshape(chans, 1)
    shift = jnp.broadcast_to(shift, (chans, 1))

    block = lax.dynamic_slice_in_dim(msa, head_id * col_width, col_width, 1)
    block = block.reshape(own_seqs, nx, ny, nz, mine, chans)
    block = block.transpose(3, 1, 2, 4, 0, 5).reshape(n_dap, mine * own_seqs, chans)
    block = lax.all_to_all(block, "dap", split_axis=0, concat_axis=0, tiled=True)

    keep = homolog.astype(F32)
    eye = jnp.eye(mine, dtype=BF16)
    right_weight = (eye[:, None, :, None] * factors[:, 1][None, :, None, :]).reshape(
        mine, chans, mine * CO
    )
    left_weight = factors[:, 0].T
    zi, xi, yi = dap_id // (nx * ny), (dap_id // ny) % nx, dap_id % ny
    start = head_id * col_width + xi * (ny * nz * mine) + yi * (nz * mine) + zi * mine
    own_amino = lax.dynamic_slice_in_dim(amino, start, mine)
    row = lambda v: v.reshape(1, chans)
    lanes = mine * CO
    rows, left, right = pl.pallas_call(
        attend_kernel,
        grid=(mine,),
        in_specs=[
            pl.BlockSpec(memory_space=pltpu.SMEM),
            pl.BlockSpec((n_dap, own_seqs, chans), lambda k: (0, k, 0)),
            whole(weights.shape),
            whole((chans, 1)),
            whole((1, chans)),
            whole((1, chans)),
            whole((1, chans)),
            whole((1, chans)),
            whole((1, chans)),
            whole((seqs, 1)),
            whole((1, seqs)),
            pl.BlockSpec((None, chans, lanes), lambda k: (k, 0, 0)),
            whole((CO, chans)),
        ],
        out_specs=[
            whole((seqs * mine, chans)),
            pl.BlockSpec((1, CO, seqs), lambda k: (k, 0, 0)),
            whole((seqs, lanes)),
        ],
        out_shape=[
            jax.ShapeDtypeStruct((seqs * mine, chans), BF16),
            jax.ShapeDtypeStruct((mine, CO, seqs), BF16),
            jax.ShapeDtypeStruct((seqs, lanes), BF16),
        ],
        scratch_shapes=[
            pltpu.VMEM((chans, seqs), BF16),
            pltpu.VMEM((seqs, chans), BF16),
            pltpu.VMEM((chans, seqs), BF16),
            pltpu.VMEM((chans, seqs), F32),
            pltpu.VMEM((chans, seqs), BF16),
            pltpu.VMEM((chans // 128, seqs * mine, 128), F32),
            pltpu.VMEM((seqs, lanes), F32),
        ],
        compiler_params=pltpu.CompilerParams(
            dimension_semantics=("arbitrary",), vmem_limit_bytes=48 * 2**20
        ),
        cost_estimate=pl.CostEstimate(
            flops=16_000_000_000, bytes_accessed=4 * 2**20, transcendentals=9_000_000
        ),
        name="attend",
    )(
        own_amino,
        block,
        weights,
        shift,
        row(gain),
        row(bias),
        row(final_bias),
        row(gain2),
        row(bias2),
        keep.reshape(seqs, 1),
        keep.reshape(1, seqs),
        right_weight,
        left_weight,
    )

    spread = jnp.broadcast_to(right[None], (n_dap, seqs, lanes))
    gathered = lax.all_to_all(spread, "dap", split_axis=0, concat_axis=0, tiled=True)

    swap = []
    for z in range(nz):
        for rest in range(nx * ny):
            for h in range(n_head):
                swap.append(
                    ((z * nx * ny + rest) * n_head + h, (h * nx * ny + rest) * n_head + z)
                )
    left = lax.ppermute(left, ("dap", "head"), swap)
    left = lax.all_gather(left, "head", axis=0, tiled=True)
    i_rows = mine * n_head
    left = jnp.swapaxes(left, 0, 1).reshape(CO * i_rows, seqs)

    back = lax.all_to_all(
        rows.reshape(n_dap * n_head, seqs * mine // (n_dap * n_head), chans),
        ("dap", "head"),
        split_axis=0,
        concat_axis=0,
        tiled=True,
    )
    own = own_seqs // n_head
    back = back.reshape(nz, nx, ny, n_head, own, mine, chans)
    alignment = back.transpose(4, 3, 1, 2, 0, 5, 6).reshape(own, residues, chans)

    depth = pair_weight.shape[1]
    wide = pair_weight.astype(BF16).reshape(CO, 1, CO, 1, depth)
    wide = (eye[None, :, None, :, None] * wide).reshape(CO * lanes, mine * depth)
    total = jnp.sum(homolog).astype(F32)
    row_keep = lax.dynamic_slice_in_dim(amino, dap_id * i_rows, i_rows).astype(F32)
    col_keep = lax.dynamic_slice_in_dim(amino, head_id * col_width, col_width).astype(F32)
    norm = jnp.maximum(
        total * row_keep[None, :, None] * col_keep.reshape(n_dap, 1, mine), 1.0
    )
    inverse = (1.0 / norm).reshape(n_dap * i_rows, mine)
    count = 4
    order = lambda b: b
    gathered = gathered.reshape(nz, nx * ny, seqs, lanes)
    pair = pl.pallas_call(
        pair_kernel,
        grid=(n_dap // count,),
        in_specs=[
            whole((CO * i_rows, seqs)),
            pl.BlockSpec((nz, None, seqs, lanes), lambda k: (0, k, 0, 0)),
            whole(wide.shape),
            whole((1, depth)),
            whole(inverse.shape),
        ],
        out_specs=whole((i_rows, col_width, depth)),
        out_shape=jax.ShapeDtypeStruct((i_rows, col_width, depth), F32),
        scratch_shapes=[pltpu.VMEM((n_dap * i_rows, CO * lanes), BF16)],
        compiler_params=pltpu.CompilerParams(
            dimension_semantics=("arbitrary",), vmem_limit_bytes=48 * 2**20
        ),
        cost_estimate=pl.CostEstimate(
            flops=5_000_000_000, bytes_accessed=10 * 2**20, transcendentals=0
        ),
        name="pair",
    )(left, gathered, wide, pair_bias.reshape(1, depth), inverse)
    return alignment, pair


def solution(mesh):
    return jax.shard_map(
        per_device,
        mesh=mesh,
        in_specs=(
            P("dap", None, None),
            P(),
            P(),
            P(),
            P(),
            P(None, None, "head"),
            P("head"),
            P("head", None),
            P(),
            P(),
            P(),
            P(),
            P(),
            P(),
        ),
        out_specs=(P(("dap", "head"), None, None), P("dap", "head", None)),
        check_vma=False,
    )
```

```python
import math

import jax
import jax.numpy as jnp
import numpy as np
from jax import lax
from jax.experimental import pallas as pl
from jax.experimental.pallas import tpu as pltpu
from jax.sharding import PartitionSpec as P

DH = 32
CO = 32
STEPS = (0, -1, 1, 2)
LOG2E = math.log2(math.e)


def bf16_terms(value):
    terms = []
    for _ in range(3):
        term = float(np.float32(value).astype(jnp.bfloat16))
        terms.append(term)
        value = float(np.float32(value)) - term
    return tuple(terms)


MASKS = bf16_terms(-1e9 * LOG2E)
NT = (((1,), (1,)), ((), ()))
TN = (((0,), (0,)), ((), ()))
F32 = jnp.float32
BF16 = jnp.bfloat16


def layer_norm(value, gain, bias):
    mean = jnp.mean(value, -1, keepdims=True)
    centred = value - mean
    spread = jnp.mean(centred * centred, -1, keepdims=True)
    return centred * lax.rsqrt(spread + 1e-05) * gain + bias


def attend_kernel(
    amino_ref,
    x_ref,
    w0_ref,
    w1_ref,
    w2_ref,
    w3_ref,
    shift_ref,
    gain_ref,
    bias_ref,
    out_bias_ref,
    gain2_ref,
    bias2_ref,
    keep_col_ref,
    keep_row_ref,
    right_weight_ref,
    left_weight_ref,
    rows_ref,
    left_ref,
    right_ref,
    q_ref,
    k_ref,
    v_ref,
    g_ref,
    a_ref,
    rows_scratch,
    right_scratch,
):
    steps = left_ref.shape[0]
    seqs = keep_col_ref.shape[0]
    w_refs = (w0_ref, w1_ref, w2_ref, w3_ref)
    chans = w0_ref.shape[1]
    width = chans // len(w_refs)
    own = seqs // x_ref.shape[0]

    def weight(which):
        return jnp.concatenate([w[which * width : (which + 1) * width, :] for w in w_refs], 0)

    absent = 1.0 - keep_col_ref[...]
    column = lax.broadcasted_iota(jnp.int32, (seqs, 128), 1) - DH
    extra = jnp.where(column == 0, MASKS[0], jnp.where(column == 1, MASKS[1], MASKS[2]))
    extra = jnp.where((column >= 0) & (column < 3), extra * absent, 0.0).astype(BF16)
    for head in range(chans // DH):
        k_ref[head] = extra
    row = lax.broadcasted_iota(jnp.int32, (16, seqs), 0)
    rest = jnp.where(row < 3, 1.0, 0.0).astype(BF16)
    ones = jnp.ones((16, seqs), BF16)

    def body(step, _):
        at = pl.multiple_of(step * own, own)
        x = x_ref[:, pl.ds(at, own), :].reshape(seqs, chans).astype(F32)
        normed = layer_norm(x, gain_ref[...], bias_ref[...]).astype(BF16)

        def transposed(which):
            return lax.dot_general(weight(which), normed, NT, preferred_element_type=F32)

        q_ref[...] = (transposed(0) * (DH**-0.5 * LOG2E)).astype(BF16)
        keys = lax.dot_general(normed, weight(1), NT, preferred_element_type=F32)
        keys = (keys * keep_col_ref[...]).astype(BF16)
        for head in range(chans // DH):
            k_ref[head, :, :DH] = keys[:, head * DH : (head + 1) * DH]
        v_ref[...] = transposed(2).astype(BF16)
        g_ref[...] = jax.nn.sigmoid(transposed(3) + shift_ref[...])

        def score(index):
            head, part = index // 1, index % 1
            cols = slice(part * (seqs // 1), (part + 1) * (seqs // 1))
            query = jnp.concatenate([q_ref[head * DH : (head + 1) * DH, cols], rest[:, cols]], 0)
            return jnp.dot(k_ref[head, :, : DH + 16], query, preferred_element_type=F32)

        def attend(index, scores):
            head, part = index // 1, index % 1
            cols = slice(part * (seqs // 1), (part + 1) * (seqs // 1))
            low, high = head * DH, (head + 1) * DH
            top = jnp.max(scores, 0, keepdims=True)
            probs = jnp.exp2(scores - top).astype(BF16)
            both = jnp.concatenate([v_ref[low:high, :], ones], 0)
            mixed = jnp.dot(both, probs, preferred_element_type=F32)
            scale = 1.0 / mixed[DH : DH + 1, :]
            a_ref[low:high, cols] = (mixed[:DH, :] * scale * g_ref[low:high, cols]).astype(BF16)

        count = chans // DH * 1
        ahead = score(0)
        for index in range(count):
            now = ahead
            if index + 1 < count:
                ahead = score(index + 1)
            attend(index, now)
        update = lax.dot_general(a_ref[...], weight(4), TN, preferred_element_type=F32)
        fresh = (x + update + out_bias_ref[...]).astype(BF16)
        wide = fresh.astype(F32)
        for part in range(chans // 128):
            rows_scratch[part, pl.ds(step, seqs, stride=steps), :] = wide[
                :, part * 128 : (part + 1) * 128
            ]
        opm = layer_norm(wide, gain2_ref[...], bias2_ref[...]).astype(BF16)
        here = amino_ref[step].astype(F32)
        left = lax.dot_general(left_weight_ref[...], opm, NT, preferred_element_type=F32)
        left_ref[step] = (left * (keep_row_ref[...] * here)).astype(BF16)
        right = jnp.dot(opm, right_weight_ref[step], preferred_element_type=F32)
        right_scratch[...] += right * (keep_col_ref[...] * here)
        return 0

    right_scratch[...] = jnp.zeros_like(right_scratch)
    lax.fori_loop(0, steps, body, 0)
    right_ref[...] = right_scratch[...].astype(BF16).reshape(right_ref.shape)
    for part in range(chans // 128):
        rows_ref[:, part * 128 : (part + 1) * 128] = rows_scratch[part].astype(BF16)


def join_kernel(*refs):
    half = (len(refs) - 2) // 2
    for colour in range(2):
        out_ref = refs[2 * half + colour]
        for index in range(half):
            piece = refs[colour * half + index]
            count = piece.shape[0]
            out_ref[index * count : (index + 1) * count] = piece[...]


def pair_kernel(
    place_ref,
    left_ref,
    bias_ref,
    inverse_ref,
    back_ref,
    compact_ref,
    z0_ref,
    z1_ref,
    z2_ref,
    z3_ref,
    x0_ref,
    x1_ref,
    x2_ref,
    x3_ref,
    out_ref,
    aligned_ref,
    mid_ref,
    weight_ref,
):
    rows = out_ref.shape[0]
    lanes = z0_ref.shape[2]

    def source(dz, dx, dy):
        first = (z0_ref, z1_ref, z2_ref, z3_ref)[dz][dx * 2 + dy]
        second = (x0_ref, x1_ref, x2_ref, x3_ref)[dx][dz * 2 + dy]
        return jnp.concatenate([first, second], 0)

    low = lax.broadcasted_iota(jnp.int32, (8, back_ref.shape[2]), 0) < 4

    def arrange(index, _):
        head, xy = index // 8, index % 8
        blocks = [
            back_ref[(z * 8 + xy) * 4 + head].astype(F32) for z in range(4)
        ]
        for upper in range(2):
            tiles = [b[upper * 8 : upper * 8 + 8] for b in blocks]
            turned = [pltpu.roll(t, 4, 0) for t in tiles]
            first = [jnp.where(low, tiles[z], turned[z + 1]) for z in (0, 2)]
            second = [jnp.where(low, turned[z], tiles[z + 1]) for z in (0, 2)]
            at = pl.multiple_of(head * 128 + xy * 16, 16)
            for seq, value in ((0, first), (1, second)):
                aligned_ref[upper * 2 + seq, pl.ds(at, 16), :] = jnp.concatenate(
                    value, 0
                ).astype(BF16)
        return 0

    lax.fori_loop(0, back_ref.shape[0] // 4, arrange, 0)
    depth = bias_ref.shape[1]
    inner = lanes // CO
    nothing = jnp.zeros((CO, depth), BF16)
    for c in range(CO):
        block = compact_ref[c * CO : (c + 1) * CO, :].astype(BF16)
        for k in range(inner):
            at = (c * inner + k) * CO
            for j in range(inner):
                weight_ref[at : at + CO, j * depth : (j + 1) * depth] = (
                    block if j == k else nothing
                )
    left = left_ref[...]
    for dz in range(4):
        for pair in range(2):
            slots = [(dz, pair * 2 + q // 2, q % 2) for q in range(4)]
            pieces = jnp.concatenate([source(*slot) for slot in slots], 1)
            outer = jnp.dot(left, pieces, preferred_element_type=F32).astype(BF16)
            for q, (z, x, y) in enumerate(slots):
                at = pl.multiple_of(place_ref[(z * 4 + x) * 2 + y] * rows, rows)
                for c in range(CO):
                    mid_ref[pl.ds(at, rows), c * lanes : (c + 1) * lanes] = outer[
                        c * rows : (c + 1) * rows, q * lanes : (q + 1) * lanes
                    ]
    blocks = mid_ref.shape[0] // rows
    for k in range(0, inner, 2):
        total = jnp.dot(
            mid_ref[...],
            weight_ref[:, k * depth : (k + 2) * depth],
            preferred_element_type=F32,
        )
        for j in range(2):
            value = total[:, j * depth : (j + 1) * depth]
            value = (value + bias_ref[...]) * inverse_ref[:, k + j : k + j + 1]
            for b in range(blocks):
                out_ref[:, b * inner + k + j, :] = value[b * rows : (b + 1) * rows]


def whole():
    return pl.BlockSpec(memory_space=pltpu.VMEM)


def per_device(
    msa,
    homolog,
    amino,
    gain,
    bias,
    focus,
    switch,
    final,
    final_bias,
    gain2,
    bias2,
    factors,
    pair_weight,
    pair_bias,
):
    n_dap, n_head = lax.axis_size("dap"), lax.axis_size("head")
    head_id, dap_id = lax.axis_index("head"), lax.axis_index("dap")
    own_seqs, residues, chans = msa.shape
    seqs = homolog.shape[0]
    width = focus.shape[2]
    col_width = residues // n_head
    mine = col_width // n_dap
    nz, nx, ny = 4, 4, 2

    parts = jnp.moveaxis(focus, 0, 2).reshape(4 * width, chans)
    first = lax.reduce_precision(switch, 8, 7)
    second = lax.reduce_precision(switch - first, 8, 7)
    third = switch - first - second
    offsets = jnp.zeros((16, chans), BF16)
    offsets = offsets.at[:3, :width].set(jnp.stack([first, second, third]).astype(BF16))
    bundle = jnp.concatenate([parts, final, offsets], 0)
    bundles = [bundle] + [
        lax.ppermute(bundle, "head", [(h, h ^ flip) for h in range(n_head)])
        for flip in range(1, n_head)
    ]
    base = 5 * width
    shift = jnp.stack([b[base : base + 3, :width] for b in bundles]).astype(F32)
    shift = ((shift[:, 0] + shift[:, 1]) + shift[:, 2]).reshape(chans, 1)

    block = lax.dynamic_slice_in_dim(msa, head_id * col_width, col_width, 1)
    block = block.reshape(own_seqs, nx, ny, nz, mine, chans)
    block = block.transpose(3, 1, 2, 4, 0, 5).reshape(n_dap, mine * own_seqs, chans)
    block = lax.all_to_all(block, "dap", split_axis=0, concat_axis=0, tiled=True)

    keep = homolog.astype(F32)
    eye = jnp.eye(mine, dtype=BF16)
    right_weight = (eye[:, None, :, None] * factors[:, 1][None, :, None, :]).reshape(
        mine, chans, mine * CO
    )
    left_weight = factors[:, 0].T
    zi, xi, yi = dap_id // (nx * ny), (dap_id // ny) % nx, dap_id % ny
    start = head_id * col_width + xi * (ny * nz * mine) + yi * (nz * mine) + zi * mine
    own_amino = lax.dynamic_slice_in_dim(amino, start, mine)
    row = lambda v: v.reshape(1, chans)
    lanes = mine * CO
    depth = pair_weight.shape[1]
    rows, left, right = pl.pallas_call(
        attend_kernel,
        in_specs=[
            pl.BlockSpec(memory_space=pltpu.SMEM),
            whole(),
            *[whole()] * n_head,
            whole(),
            whole(),
            whole(),
            whole(),
            whole(),
            whole(),
            whole(),
            whole(),
            whole(),
            whole(),
        ],
        out_specs=[whole(), whole(), whole()],
        out_shape=[
            jax.ShapeDtypeStruct((seqs * mine, chans), BF16),
            jax.ShapeDtypeStruct((mine, CO, seqs), BF16),
            jax.ShapeDtypeStruct((2, seqs // 2, lanes), BF16),
        ],
        scratch_shapes=[
            pltpu.VMEM((chans, seqs), BF16),
            pltpu.VMEM((chans // DH, seqs, 128), BF16),
            pltpu.VMEM((chans, seqs), BF16),
            pltpu.VMEM((chans, seqs), F32),
            pltpu.VMEM((chans, seqs), BF16),
            pltpu.VMEM((chans // 128, seqs * mine, 128), F32),
            pltpu.VMEM((seqs, lanes), F32),
        ],
        compiler_params=pltpu.CompilerParams(
            vmem_limit_bytes=24 * 2**20
        ),
        cost_estimate=pl.CostEstimate(
            flops=16_000_000_000, bytes_accessed=4 * 2**20, transcendentals=9_000_000
        ),
        name="attend",
    )(
        own_amino,
        block,
        *bundles,
        shift,
        row(gain),
        row(bias),
        row(final_bias),
        row(gain2),
        row(bias2),
        keep.reshape(seqs, 1),
        keep.reshape(1, seqs),
        right_weight,
        left_weight,
    )

    swap = []
    for z in range(nz):
        for rest in range(nx * ny):
            for h in range(n_head):
                swap.append(
                    ((z * nx * ny + rest) * n_head + h, (h * nx * ny + rest) * n_head + z)
                )
    left = lax.ppermute(left, ("dap", "head"), swap)

    def shifted(value, axis, by):
        pairs = []
        for z in range(nz):
            for x in range(nx):
                for y in range(ny):
                    to = [z, x, y]
                    to[axis] = (to[axis] + by) % (nz, nx, ny)[axis]
                    pairs.append(((z * nx + x) * ny + y, (to[0] * nx + to[1]) * ny + to[2]))
        return lax.ppermute(value, "dap", pairs)

    other = shifted(right, 2, 1)

    def first_stage(value, axis):
        return [value] + [shifted(value, axis, -step) for step in STEPS[1:]]

    def second_stage(value, axis):
        from_left, from_right = shifted(value, axis, 1), shifted(value, axis, -1)
        return value, from_left, from_right

    colours = [jnp.stack([right[part], other[part]]) for part in range(2)]
    parts = first_stage(colours[0], 1) + first_stage(colours[1], 0)
    shape = (len(STEPS) * ny, *parts[0].shape[1:])
    mids = pl.pallas_call(
        join_kernel,
        in_specs=[pl.BlockSpec(memory_space=pltpu.VMEM)] * len(parts),
        out_specs=[pl.BlockSpec(memory_space=pltpu.VMEM)] * 2,
        out_shape=[jax.ShapeDtypeStruct(shape, BF16)] * 2,
        compiler_params=pltpu.CompilerParams(vmem_limit_bytes=4 * 2**20),
        cost_estimate=pl.CostEstimate(
            flops=2_000_000, bytes_accessed=2 * 2**20, transcendentals=0
        ),
        name="join",
    )(*parts)
    (*mids, left, rows) = lax.optimization_barrier((*mids, left, rows))
    z_pieces = second_stage(mids[0], 0)
    x_pieces = second_stage(mids[1], 1)
    z_pieces = (*z_pieces, shifted(z_pieces[1], 0, 1))
    x_pieces = (*x_pieces, shifted(x_pieces[1], 1, 1))

    left = lax.all_gather(left, "head", axis=0, tiled=True)
    i_rows = mine * n_head
    left = jnp.swapaxes(left, 0, 1).reshape(CO * i_rows, seqs)

    back = lax.all_to_all(
        rows.reshape(n_dap * n_head, seqs * mine // (n_dap * n_head), chans),
        ("dap", "head"),
        split_axis=0,
        concat_axis=0,
        tiled=True,
    )
    own = own_seqs // n_head
    total = jnp.sum(homolog).astype(F32)
    row_keep = lax.dynamic_slice_in_dim(amino, dap_id * i_rows, i_rows).astype(F32)
    col_keep = lax.dynamic_slice_in_dim(amino, head_id * col_width, col_width).astype(F32)
    norm = jnp.maximum(
        total * row_keep[None, :, None] * col_keep.reshape(n_dap, 1, mine), 1.0
    )
    inverse = (1.0 / norm).reshape(n_dap * i_rows, mine)
    places = []
    for dz in STEPS:
        for dx in STEPS:
            for dy in range(ny):
                at_z, at_x, at_y = (zi + dz) % nz, (xi + dx) % nx, (yi + dy) % ny
                places.append((at_x * ny + at_y) * nz + at_z)
    pieces = (*z_pieces, *x_pieces)
    pair, alignment = pl.pallas_call(
        pair_kernel,
        in_specs=[
            pl.BlockSpec(memory_space=pltpu.SMEM),
            *[pl.BlockSpec(memory_space=pltpu.VMEM)] * (5 + len(pieces)),
        ],
        out_specs=[pl.BlockSpec(memory_space=pltpu.VMEM)] * 2,
        out_shape=[
            jax.ShapeDtypeStruct((i_rows, col_width, depth), F32),
            jax.ShapeDtypeStruct((own, residues, chans), BF16),
        ],
        scratch_shapes=[
            pltpu.VMEM((n_dap * i_rows, CO * lanes), BF16),
            pltpu.VMEM((CO * lanes, mine * depth), BF16),
        ],
        compiler_params=pltpu.CompilerParams(vmem_limit_bytes=18 * 2**20),
        cost_estimate=pl.CostEstimate(
            flops=5_000_000_000, bytes_accessed=10 * 2**20, transcendentals=0
        ),
        name="pair",
    )(
        jnp.stack(places).astype(jnp.int32),
        left,
        pair_bias.reshape(1, depth),
        inverse,
        back,
        pair_weight,
        *pieces,
    )
    return alignment, pair


def solution(mesh):
    return jax.shard_map(
        per_device,
        mesh=mesh,
        in_specs=(
            P("dap", None, None),
            P(),
            P(),
            P(),
            P(),
            P(None, None, "head"),
            P("head"),
            P("head", None),
            P(),
            P(),
            P(),
            P(),
            P(),
            P(),
        ),
        out_specs=(P(("dap", "head"), None, None), P("dap", "head", None)),
        check_vma=False,
    )
```

```python
import math

import jax
import jax.numpy as jnp
import numpy as np
from jax import lax
from jax.experimental import pallas as pl
from jax.experimental.pallas import tpu as pltpu
from jax.sharding import PartitionSpec as P

DH = 32
CO = 32
STEPS = (0, -1, 1, 2)
LOG2E = math.log2(math.e)


def bf16_terms(value):
    terms = []
    for _ in range(3):
        term = float(np.float32(value).astype(jnp.bfloat16))
        terms.append(term)
        value = float(np.float32(value)) - term
    return tuple(terms)


MASKS = bf16_terms(-1e9 * LOG2E)
NT = (((1,), (1,)), ((), ()))
TN = (((0,), (0,)), ((), ()))
F32 = jnp.float32
BF16 = jnp.bfloat16


def layer_norm(value, gain, bias):
    mean = jnp.mean(value, -1, keepdims=True)
    centred = value - mean
    spread = jnp.mean(centred * centred, -1, keepdims=True)
    return centred * lax.rsqrt(spread + 1e-05) * gain + bias


def attend_kernel(
    amino_ref,
    x_ref,
    w0_ref,
    w1_ref,
    w2_ref,
    w3_ref,
    shift_ref,
    gain_ref,
    bias_ref,
    out_bias_ref,
    gain2_ref,
    bias2_ref,
    keep_col_ref,
    keep_row_ref,
    right_weight_ref,
    left_weight_ref,
    rows_ref,
    left_ref,
    right_ref,
    q_ref,
    k_ref,
    v_ref,
    g_ref,
    a_ref,
    rows_scratch,
    right_scratch,
):
    steps = left_ref.shape[0]
    seqs = keep_col_ref.shape[0]
    w_refs = (w0_ref, w1_ref, w2_ref, w3_ref)
    chans = w0_ref.shape[1]
    width = chans // len(w_refs)
    own = seqs // x_ref.shape[0]

    def weight(which):
        return jnp.concatenate([w[which * width : (which + 1) * width, :] for w in w_refs], 0)

    absent = 1.0 - keep_col_ref[...]
    column = lax.broadcasted_iota(jnp.int32, (seqs, 128), 1) - DH
    extra = jnp.where(column == 0, MASKS[0], jnp.where(column == 1, MASKS[1], MASKS[2]))
    extra = jnp.where((column >= 0) & (column < 3), extra * absent, 0.0).astype(BF16)
    for head in range(chans // DH):
        k_ref[head] = extra
    row = lax.broadcasted_iota(jnp.int32, (16, seqs), 0)
    rest = jnp.where(row < 3, 1.0, 0.0).astype(BF16)
    ones = jnp.ones((16, seqs), BF16)

    def body(step, _):
        at = pl.multiple_of(step * own, own)
        x = x_ref[:, pl.ds(at, own), :].reshape(seqs, chans).astype(F32)
        normed = layer_norm(x, gain_ref[...], bias_ref[...]).astype(BF16)

        def transposed(which):
            return lax.dot_general(weight(which), normed, NT, preferred_element_type=F32)

        q_ref[...] = (transposed(0) * (DH**-0.5 * LOG2E)).astype(BF16)
        keys = lax.dot_general(normed, weight(1), NT, preferred_element_type=F32)
        keys = (keys * keep_col_ref[...]).astype(BF16)
        for head in range(chans // DH):
            k_ref[head, :, :DH] = keys[:, head * DH : (head + 1) * DH]
        v_ref[...] = transposed(2).astype(BF16)
        g_ref[...] = jax.nn.sigmoid(transposed(3) + shift_ref[...])

        def score(index):
            head, part = index // 1, index % 1
            cols = slice(part * (seqs // 1), (part + 1) * (seqs // 1))
            query = jnp.concatenate([q_ref[head * DH : (head + 1) * DH, cols], rest[:, cols]], 0)
            return jnp.dot(k_ref[head, :, : DH + 16], query, preferred_element_type=F32)

        def attend(index, scores):
            head, part = index // 1, index % 1
            cols = slice(part * (seqs // 1), (part + 1) * (seqs // 1))
            low, high = head * DH, (head + 1) * DH
            top = jnp.max(scores, 0, keepdims=True)
            probs = jnp.exp2(scores - top).astype(BF16)
            both = jnp.concatenate([v_ref[low:high, :], ones], 0)
            mixed = jnp.dot(both, probs, preferred_element_type=F32)
            scale = 1.0 / mixed[DH : DH + 1, :]
            a_ref[low:high, cols] = (mixed[:DH, :] * scale * g_ref[low:high, cols]).astype(BF16)

        count = chans // DH * 1
        ahead = score(0)
        for index in range(count):
            now = ahead
            if index + 1 < count:
                ahead = score(index + 1)
            attend(index, now)
        update = lax.dot_general(a_ref[...], weight(4), TN, preferred_element_type=F32)
        fresh = (x + update + out_bias_ref[...]).astype(BF16)
        wide = fresh.astype(F32)
        for part in range(chans // 128):
            rows_scratch[part, pl.ds(step, seqs, stride=steps), :] = wide[
                :, part * 128 : (part + 1) * 128
            ]
        opm = layer_norm(wide, gain2_ref[...], bias2_ref[...]).astype(BF16)
        here = amino_ref[step].astype(F32)
        left = lax.dot_general(left_weight_ref[...], opm, NT, preferred_element_type=F32)
        left_ref[step] = (left * (keep_row_ref[...] * here)).astype(BF16)
        right = jnp.dot(opm, right_weight_ref[step], preferred_element_type=F32)
        right_scratch[...] += right * (keep_col_ref[...] * here)
        return 0

    right_scratch[...] = jnp.zeros_like(right_scratch)
    lax.fori_loop(0, steps, body, 0)
    right_ref[...] = right_scratch[...].astype(BF16).reshape(right_ref.shape)
    for part in range(chans // 128):
        rows_ref[:, part * 128 : (part + 1) * 128] = rows_scratch[part].astype(BF16)


def join_kernel(*refs):
    half = (len(refs) - 2) // 2
    for colour in range(2):
        out_ref = refs[2 * half + colour]
        for index in range(half):
            piece = refs[colour * half + index]
            count = piece.shape[0]
            out_ref[index * count : (index + 1) * count] = piece[...]


def project(slots, groups, z_refs, x_refs, left_ref, bias_ref, inverse_ref, compact_ref,
            place_ref, mid_ref, weight_ref, store):
    lanes = z_refs[0].shape[2]
    depth = bias_ref.shape[1]
    inner = lanes // CO
    rows = left_ref.shape[0] // CO
    nothing = jnp.zeros((CO, depth), BF16)
    for c in range(CO):
        block = compact_ref[c * CO : (c + 1) * CO, :].astype(BF16)
        for k in range(inner):
            at = (c * inner + k) * CO
            for j in range(inner):
                weight_ref[at : at + CO, j * depth : (j + 1) * depth] = (
                    block if j == k else nothing
                )

    def source(dz, dx, dy):
        return jnp.concatenate([z_refs[dz][dx * 2 + dy], x_refs[dx][dz * 2 + dy]], 0)

    left = left_ref[...]
    size = len(slots) // groups
    for group in range(groups):
        batch = slots[group * size : (group + 1) * size]
        pieces = jnp.concatenate([source(*slot) for slot in batch], 1)
        outer = jnp.dot(left, pieces, preferred_element_type=F32).astype(BF16)
        for q in range(size):
            at = (group * size + q) * rows
            for c in range(CO):
                mid_ref[at : at + rows, c * lanes : (c + 1) * lanes] = outer[
                    c * rows : (c + 1) * rows, q * lanes : (q + 1) * lanes
                ]
    for k in range(0, inner, 2):
        total = jnp.dot(
            mid_ref[...],
            weight_ref[:, k * depth : (k + 2) * depth],
            preferred_element_type=F32,
        )
        for n, (dz, dx, dy) in enumerate(slots):
            place = place_ref[(dz * 4 + dx) * 2 + dy]
            inverse = inverse_ref[pl.ds(pl.multiple_of(place * rows, rows), rows), :]
            for j in range(2):
                value = total[n * rows : (n + 1) * rows, j * depth : (j + 1) * depth]
                value = (value + bias_ref[...]) * inverse[:, k + j : k + j + 1]
                store(n, place, k + j, value)


EARLY = tuple((dz, dx, dy) for dz in range(3) for dx in range(3) for dy in range(2))
LATE = tuple(
    (dz, dx, dy) for dz in range(4) for dx in range(4) for dy in range(2) if 3 in (dz, dx)
)


def early_kernel(
    place_ref,
    left_ref,
    bias_ref,
    inverse_ref,
    compact_ref,
    back_ref,
    z0_ref,
    z1_ref,
    z2_ref,
    x0_ref,
    x1_ref,
    x2_ref,
    part_ref,
    aligned_ref,
    mid_ref,
    weight_ref,
):
    low = lax.broadcasted_iota(jnp.int32, (8, back_ref.shape[2]), 0) < 4

    def arrange(index, _):
        head, xy = index // 8, index % 8
        blocks = [back_ref[(z * 8 + xy) * 4 + head].astype(F32) for z in range(4)]
        for upper in range(2):
            tiles = [b[upper * 8 : upper * 8 + 8] for b in blocks]
            turned = [pltpu.roll(t, 4, 0) for t in tiles]
            first = [jnp.where(low, tiles[z], turned[z + 1]) for z in (0, 2)]
            second = [jnp.where(low, turned[z], tiles[z + 1]) for z in (0, 2)]
            at = pl.multiple_of(head * 128 + xy * 16, 16)
            for seq, value in ((0, first), (1, second)):
                aligned_ref[upper * 2 + seq, pl.ds(at, 16), :] = jnp.concatenate(
                    value, 0
                ).astype(BF16)
        return 0

    lax.fori_loop(0, back_ref.shape[0] // 4, arrange, 0)
    rows = left_ref.shape[0] // CO
    inner = z0_ref.shape[2] // CO

    def store(n, place, k, value):
        at = (n * inner + k) * rows
        part_ref[at : at + rows, :] = value

    project(EARLY, 3, (z0_ref, z1_ref, z2_ref), (x0_ref, x1_ref, x2_ref), left_ref, bias_ref,
            inverse_ref, compact_ref, place_ref, mid_ref, weight_ref, store)


def late_kernel(
    place_ref,
    left_ref,
    bias_ref,
    inverse_ref,
    compact_ref,
    part_ref,
    z0_ref,
    z1_ref,
    z2_ref,
    z3_ref,
    x0_ref,
    x1_ref,
    x2_ref,
    x3_ref,
    out_ref,
    mid_ref,
    weight_ref,
    turn_ref,
):
    rows = left_ref.shape[0] // CO
    inner = z0_ref.shape[2] // CO

    def store(n, place, k, value):
        at = pl.multiple_of((place * inner + k) * rows, rows)
        turn_ref[pl.ds(at, rows), :] = value

    project(LATE, 2, (z0_ref, z1_ref, z2_ref, z3_ref), (x0_ref, x1_ref, x2_ref, x3_ref),
            left_ref, bias_ref, inverse_ref, compact_ref, place_ref, mid_ref, weight_ref, store)
    block = inner * rows
    for n, (dz, dx, dy) in enumerate(EARLY):
        at = pl.multiple_of(place_ref[(dz * 4 + dx) * 2 + dy] * block, block)
        turn_ref[pl.ds(at, block), :] = part_ref[n * block : (n + 1) * block, :]
    columns = out_ref.shape[1]
    for i in range(rows):
        out_ref[i] = turn_ref[pl.ds(i, columns, stride=rows), :]


def whole():
    return pl.BlockSpec(memory_space=pltpu.VMEM)


def per_device(
    msa,
    homolog,
    amino,
    gain,
    bias,
    focus,
    switch,
    final,
    final_bias,
    gain2,
    bias2,
    factors,
    pair_weight,
    pair_bias,
):
    n_dap, n_head = lax.axis_size("dap"), lax.axis_size("head")
    head_id, dap_id = lax.axis_index("head"), lax.axis_index("dap")
    own_seqs, residues, chans = msa.shape
    seqs = homolog.shape[0]
    width = focus.shape[2]
    col_width = residues // n_head
    mine = col_width // n_dap
    nz, nx, ny = 4, 4, 2

    parts = jnp.moveaxis(focus, 0, 2).reshape(4 * width, chans)
    first = lax.reduce_precision(switch, 8, 7)
    second = lax.reduce_precision(switch - first, 8, 7)
    third = switch - first - second
    offsets = jnp.zeros((16, chans), BF16)
    offsets = offsets.at[:3, :width].set(jnp.stack([first, second, third]).astype(BF16))
    bundle = jnp.concatenate([parts, final, offsets], 0)
    swap_core = [(h, h ^ 1) for h in range(n_head)]
    across = [
        (d * n_head + h, (d ^ 1) * n_head + (h ^ 2))
        for d in range(n_dap)
        for h in range(n_head)
    ]
    far_bundle = lax.ppermute(bundle, ("dap", "head"), across)
    bundles = [
        bundle,
        lax.ppermute(bundle, "head", swap_core),
        far_bundle,
        lax.ppermute(far_bundle, "head", swap_core),
    ]
    base = 5 * width
    shift = jnp.stack([b[base : base + 3, :width] for b in bundles]).astype(F32)
    shift = ((shift[:, 0] + shift[:, 1]) + shift[:, 2]).reshape(chans, 1)

    block = lax.dynamic_slice_in_dim(msa, head_id * col_width, col_width, 1)
    block = block.reshape(own_seqs, nx, ny, nz, mine, chans)
    block = block.transpose(3, 1, 2, 4, 0, 5).reshape(n_dap, mine * own_seqs, chans)
    block = lax.all_to_all(block, "dap", split_axis=0, concat_axis=0, tiled=True)

    keep = homolog.astype(F32)
    eye = jnp.eye(mine, dtype=BF16)
    right_weight = (eye[:, None, :, None] * factors[:, 1][None, :, None, :]).reshape(
        mine, chans, mine * CO
    )
    left_weight = factors[:, 0].T
    zi, xi, yi = dap_id // (nx * ny), (dap_id // ny) % nx, dap_id % ny
    start = head_id * col_width + xi * (ny * nz * mine) + yi * (nz * mine) + zi * mine
    own_amino = lax.dynamic_slice_in_dim(amino, start, mine)
    row = lambda v: v.reshape(1, chans)
    lanes = mine * CO
    depth = pair_weight.shape[1]
    rows, left, right = pl.pallas_call(
        attend_kernel,
        in_specs=[
            pl.BlockSpec(memory_space=pltpu.SMEM),
            whole(),
            *[whole()] * n_head,
            whole(),
            whole(),
            whole(),
            whole(),
            whole(),
            whole(),
            whole(),
            whole(),
            whole(),
            whole(),
        ],
        out_specs=[whole(), whole(), whole()],
        out_shape=[
            jax.ShapeDtypeStruct((seqs * mine, chans), BF16),
            jax.ShapeDtypeStruct((mine, CO, seqs), BF16),
            jax.ShapeDtypeStruct((2, seqs // 2, lanes), BF16),
        ],
        scratch_shapes=[
            pltpu.VMEM((chans, seqs), BF16),
            pltpu.VMEM((chans // DH, seqs, 128), BF16),
            pltpu.VMEM((chans, seqs), BF16),
            pltpu.VMEM((chans, seqs), F32),
            pltpu.VMEM((chans, seqs), BF16),
            pltpu.VMEM((chans // 128, seqs * mine, 128), F32),
            pltpu.VMEM((seqs, lanes), F32),
        ],
        compiler_params=pltpu.CompilerParams(
            vmem_limit_bytes=24 * 2**20
        ),
        cost_estimate=pl.CostEstimate(
            flops=16_000_000_000, bytes_accessed=4 * 2**20, transcendentals=9_000_000
        ),
        name="attend",
    )(
        own_amino,
        block,
        *bundles,
        shift,
        row(gain),
        row(bias),
        row(final_bias),
        row(gain2),
        row(bias2),
        keep.reshape(seqs, 1),
        keep.reshape(1, seqs),
        right_weight,
        left_weight,
    )

    swap = []
    for z in range(nz):
        for rest in range(nx * ny):
            for h in range(n_head):
                swap.append(
                    ((z * nx * ny + rest) * n_head + h, (h * nx * ny + rest) * n_head + z)
                )
    left = lax.ppermute(left, ("dap", "head"), swap)

    def shifted(value, axis, by):
        pairs = []
        for z in range(nz):
            for x in range(nx):
                for y in range(ny):
                    to = [z, x, y]
                    to[axis] = (to[axis] + by) % (nz, nx, ny)[axis]
                    pairs.append(((z * nx + x) * ny + y, (to[0] * nx + to[1]) * ny + to[2]))
        return lax.ppermute(value, "dap", pairs)

    other = shifted(right, 2, 1)

    def first_stage(value, axis):
        return [value] + [shifted(value, axis, -step) for step in STEPS[1:]]

    def second_stage(value, axis):
        from_left, from_right = shifted(value, axis, 1), shifted(value, axis, -1)
        return value, from_left, from_right

    colours = [jnp.stack([right[part], other[part]]) for part in range(2)]
    parts = first_stage(colours[0], 1) + first_stage(colours[1], 0)
    shape = (len(STEPS) * ny, *parts[0].shape[1:])
    mids = pl.pallas_call(
        join_kernel,
        in_specs=[pl.BlockSpec(memory_space=pltpu.VMEM)] * len(parts),
        out_specs=[pl.BlockSpec(memory_space=pltpu.VMEM)] * 2,
        out_shape=[jax.ShapeDtypeStruct(shape, BF16)] * 2,
        compiler_params=pltpu.CompilerParams(vmem_limit_bytes=4 * 2**20),
        cost_estimate=pl.CostEstimate(
            flops=2_000_000, bytes_accessed=2 * 2**20, transcendentals=0
        ),
        name="join",
    )(*parts)
    (*mids, left, rows) = lax.optimization_barrier((*mids, left, rows))
    z_pieces = second_stage(mids[0], 0)
    x_pieces = second_stage(mids[1], 1)
    z_pieces = (*z_pieces, shifted(z_pieces[1], 0, 1))
    x_pieces = (*x_pieces, shifted(x_pieces[1], 1, 1))

    left = lax.all_gather(left, "head", axis=0, tiled=True)
    i_rows = mine * n_head
    left = jnp.swapaxes(left, 0, 1).reshape(CO * i_rows, seqs)

    back = lax.all_to_all(
        rows.reshape(n_dap * n_head, seqs * mine // (n_dap * n_head), chans),
        ("dap", "head"),
        split_axis=0,
        concat_axis=0,
        tiled=True,
    )
    own = own_seqs // n_head
    total = jnp.sum(homolog).astype(F32)
    row_keep = lax.dynamic_slice_in_dim(amino, dap_id * i_rows, i_rows).astype(F32)
    col_keep = lax.dynamic_slice_in_dim(amino, head_id * col_width, col_width).astype(F32)
    norm = jnp.maximum(
        total * row_keep[None, :, None] * col_keep.reshape(n_dap, 1, mine), 1.0
    )
    inverse = (1.0 / norm).reshape(n_dap * i_rows, mine)
    places = []
    for dz in STEPS:
        for dx in STEPS:
            for dy in range(ny):
                at_z, at_x, at_y = (zi + dz) % nz, (xi + dx) % nx, (yi + dy) % ny
                places.append((at_x * ny + at_y) * nz + at_z)
    shared = (
        jnp.stack(places).astype(jnp.int32),
        left,
        pair_bias.reshape(1, depth),
        inverse,
        pair_weight,
    )
    early, alignment = pl.pallas_call(
        early_kernel,
        in_specs=[
            pl.BlockSpec(memory_space=pltpu.SMEM),
            *[pl.BlockSpec(memory_space=pltpu.VMEM)] * 11,
        ],
        out_specs=[pl.BlockSpec(memory_space=pltpu.VMEM)] * 2,
        out_shape=[
            jax.ShapeDtypeStruct((len(EARLY) * mine * i_rows, depth), F32),
            jax.ShapeDtypeStruct((own, residues, chans), BF16),
        ],
        scratch_shapes=[
            pltpu.VMEM((len(EARLY) * i_rows, CO * lanes), BF16),
            pltpu.VMEM((CO * lanes, mine * depth), BF16),
        ],
        compiler_params=pltpu.CompilerParams(vmem_limit_bytes=18 * 2**20),
        cost_estimate=pl.CostEstimate(
            flops=3_000_000_000, bytes_accessed=6 * 2**20, transcendentals=0
        ),
        name="early",
    )(*shared, back, *z_pieces[:3], *x_pieces[:3])
    pair = pl.pallas_call(
        late_kernel,
        in_specs=[
            pl.BlockSpec(memory_space=pltpu.SMEM),
            *[pl.BlockSpec(memory_space=pltpu.VMEM)] * 13,
        ],
        out_specs=pl.BlockSpec(memory_space=pltpu.VMEM),
        out_shape=jax.ShapeDtypeStruct((i_rows, col_width, depth), F32),
        scratch_shapes=[
            pltpu.VMEM((len(LATE) * i_rows, CO * lanes), BF16),
            pltpu.VMEM((CO * lanes, mine * depth), BF16),
            pltpu.VMEM((col_width * i_rows, depth), F32),
        ],
        compiler_params=pltpu.CompilerParams(vmem_limit_bytes=18 * 2**20),
        cost_estimate=pl.CostEstimate(
            flops=3_000_000_000, bytes_accessed=6 * 2**20, transcendentals=0
        ),
        name="late",
    )(*shared, early, *z_pieces, *x_pieces)
    return alignment, pair


def solution(mesh):
    return jax.shard_map(
        per_device,
        mesh=mesh,
        in_specs=(
            P("dap", None, None),
            P(),
            P(),
            P(),
            P(),
            P(None, None, "head"),
            P("head"),
            P("head", None),
            P(),
            P(),
            P(),
            P(),
            P(),
            P(),
        ),
        out_specs=(P(("dap", "head"), None, None), P("dap", "head", None)),
        check_vma=False,
    )
```

```python
import math

import jax
import jax.numpy as jnp
import numpy as np
from jax import lax
from jax.experimental import pallas as pl
from jax.experimental.pallas import tpu as pltpu
from jax.sharding import PartitionSpec as P

DH = 32
CO = 32
STEPS = (0, -1, 1, 2)
LOG2E = math.log2(math.e)


def bf16_terms(value):
    terms = []
    for _ in range(3):
        term = float(np.float32(value).astype(jnp.bfloat16))
        terms.append(term)
        value = float(np.float32(value)) - term
    return tuple(terms)


MASKS = bf16_terms(-1e9 * LOG2E)
NT = (((1,), (1,)), ((), ()))
TN = (((0,), (0,)), ((), ()))
F32 = jnp.float32
BF16 = jnp.bfloat16


def layer_norm(value, gain, bias):
    mean = jnp.mean(value, -1, keepdims=True)
    centred = value - mean
    spread = jnp.mean(centred * centred, -1, keepdims=True)
    return centred * lax.rsqrt(spread + 1e-05) * gain + bias


def attend_kernel(
    amino_ref,
    x_ref,
    w0_ref,
    w1_ref,
    w2_ref,
    w3_ref,
    shift_ref,
    gain_ref,
    bias_ref,
    out_bias_ref,
    gain2_ref,
    bias2_ref,
    keep_col_ref,
    keep_row_ref,
    right_weight_ref,
    left_weight_ref,
    rows_ref,
    left_ref,
    right_ref,
    q_ref,
    k_ref,
    v_ref,
    g_ref,
    a_ref,
    rows_scratch,
    right_scratch,
):
    steps = left_ref.shape[0]
    seqs = keep_col_ref.shape[0]
    w_refs = (w0_ref, w1_ref, w2_ref, w3_ref)
    chans = w0_ref.shape[1]
    width = chans // len(w_refs)
    own = seqs // x_ref.shape[0]

    def weight(which):
        return jnp.concatenate([w[which * width : (which + 1) * width, :] for w in w_refs], 0)

    absent = 1.0 - keep_col_ref[...]
    column = lax.broadcasted_iota(jnp.int32, (seqs, 128), 1) - DH
    extra = jnp.where(column == 0, MASKS[0], jnp.where(column == 1, MASKS[1], MASKS[2]))
    extra = jnp.where((column >= 0) & (column < 3), extra * absent, 0.0).astype(BF16)
    for head in range(chans // DH):
        k_ref[head] = extra
    row = lax.broadcasted_iota(jnp.int32, (16, seqs), 0)
    rest = jnp.where(row < 3, 1.0, 0.0).astype(BF16)
    ones = jnp.ones((16, seqs), BF16)

    def body(step, _):
        at = pl.multiple_of(step * own, own)
        x = x_ref[:, pl.ds(at, own), :].reshape(seqs, chans).astype(F32)
        normed = layer_norm(x, gain_ref[...], bias_ref[...]).astype(BF16)

        def transposed(which):
            return lax.dot_general(weight(which), normed, NT, preferred_element_type=F32)

        q_ref[...] = (transposed(0) * (DH**-0.5 * LOG2E)).astype(BF16)
        keys = lax.dot_general(normed, weight(1), NT, preferred_element_type=F32)
        keys = (keys * keep_col_ref[...]).astype(BF16)
        for head in range(chans // DH):
            k_ref[head, :, :DH] = keys[:, head * DH : (head + 1) * DH]
        v_ref[...] = transposed(2).astype(BF16)
        g_ref[...] = jax.nn.sigmoid(transposed(3) + shift_ref[...])

        def score(index):
            head, part = index // 1, index % 1
            cols = slice(part * (seqs // 1), (part + 1) * (seqs // 1))
            query = jnp.concatenate([q_ref[head * DH : (head + 1) * DH, cols], rest[:, cols]], 0)
            return jnp.dot(k_ref[head, :, : DH + 16], query, preferred_element_type=F32)

        def attend(index, scores):
            head, part = index // 1, index % 1
            cols = slice(part * (seqs // 1), (part + 1) * (seqs // 1))
            low, high = head * DH, (head + 1) * DH
            top = jnp.max(scores, 0, keepdims=True)
            probs = jnp.exp2(scores - top).astype(BF16)
            both = jnp.concatenate([v_ref[low:high, :], ones], 0)
            mixed = jnp.dot(both, probs, preferred_element_type=F32)
            scale = 1.0 / mixed[DH : DH + 1, :]
            a_ref[low:high, cols] = (mixed[:DH, :] * scale * g_ref[low:high, cols]).astype(BF16)

        count = chans // DH * 1
        ahead = score(0)
        for index in range(count):
            now = ahead
            if index + 1 < count:
                ahead = score(index + 1)
            attend(index, now)
        update = lax.dot_general(a_ref[...], weight(4), TN, preferred_element_type=F32)
        fresh = (x + update + out_bias_ref[...]).astype(BF16)
        wide = fresh.astype(F32)
        for part in range(chans // 128):
            rows_scratch[part, pl.ds(step, seqs, stride=steps), :] = wide[
                :, part * 128 : (part + 1) * 128
            ]
        opm = layer_norm(wide, gain2_ref[...], bias2_ref[...]).astype(BF16)
        here = amino_ref[step].astype(F32)
        left = lax.dot_general(left_weight_ref[...], opm, NT, preferred_element_type=F32)
        left_ref[step] = (left * (keep_row_ref[...] * here)).astype(BF16)
        right = jnp.dot(opm, right_weight_ref[step], preferred_element_type=F32)
        right_scratch[...] += right * (keep_col_ref[...] * here)
        return 0

    right_scratch[...] = jnp.zeros_like(right_scratch)
    lax.fori_loop(0, steps, body, 0)
    right_ref[...] = right_scratch[...].astype(BF16).reshape(right_ref.shape)
    for part in range(chans // 128):
        rows_ref[:, part * 128 : (part + 1) * 128] = rows_scratch[part].astype(BF16)


def join_kernel(*refs):
    half = (len(refs) - 2) // 2
    for colour in range(2):
        out_ref = refs[2 * half + colour]
        for index in range(half):
            piece = refs[colour * half + index]
            count = piece.shape[0]
            out_ref[index * count : (index + 1) * count] = piece[...]


def project(slots, groups, z_refs, x_refs, left_ref, bias_ref, inverse_ref, compact_ref,
            place_ref, mid_ref, weight_ref, store):
    lanes = z_refs[0].shape[2]
    depth = bias_ref.shape[1]
    inner = lanes // CO
    rows = left_ref.shape[0] // CO
    nothing = jnp.zeros((CO, depth), BF16)
    for c in range(CO):
        block = compact_ref[c * CO : (c + 1) * CO, :].astype(BF16)
        for k in range(inner):
            at = (c * inner + k) * CO
            for j in range(inner):
                weight_ref[at : at + CO, j * depth : (j + 1) * depth] = (
                    block if j == k else nothing
                )

    def source(dz, dx, dy):
        return jnp.concatenate([z_refs[dz][dx * 2 + dy], x_refs[dx][dz * 2 + dy]], 0)

    left = left_ref[...]
    size = len(slots) // groups
    for group in range(groups):
        batch = slots[group * size : (group + 1) * size]
        pieces = jnp.concatenate([source(*slot) for slot in batch], 1)
        outer = jnp.dot(left, pieces, preferred_element_type=F32).astype(BF16)
        for q in range(size):
            at = (group * size + q) * rows
            for c in range(CO):
                mid_ref[at : at + rows, c * lanes : (c + 1) * lanes] = outer[
                    c * rows : (c + 1) * rows, q * lanes : (q + 1) * lanes
                ]
    for k in range(0, inner, 2):
        total = jnp.dot(
            mid_ref[...],
            weight_ref[:, k * depth : (k + 2) * depth],
            preferred_element_type=F32,
        )
        for n, (dz, dx, dy) in enumerate(slots):
            place = place_ref[(dz * 4 + dx) * 2 + dy]
            inverse = inverse_ref[pl.ds(pl.multiple_of(place * rows, rows), rows), :]
            for j in range(2):
                value = total[n * rows : (n + 1) * rows, j * depth : (j + 1) * depth]
                value = (value + bias_ref[...]) * inverse[:, k + j : k + j + 1]
                store(n, place, k + j, value)


EARLY = tuple((dz, dx, dy) for dz in range(3) for dx in range(3) for dy in range(2))
LATE = tuple(
    (dz, dx, dy) for dz in range(4) for dx in range(4) for dy in range(2) if 3 in (dz, dx)
)


def arrange_kernel(back_ref, aligned_ref):
    low = lax.broadcasted_iota(jnp.int32, (8, back_ref.shape[2]), 0) < 4

    def arrange(index, _):
        head, xy = index // 8, index % 8
        blocks = [back_ref[(z * 8 + xy) * 4 + head].astype(F32) for z in range(4)]
        for upper in range(2):
            tiles = [b[upper * 8 : upper * 8 + 8] for b in blocks]
            turned = [pltpu.roll(t, 4, 0) for t in tiles]
            first = [jnp.where(low, tiles[z], turned[z + 1]) for z in (0, 2)]
            second = [jnp.where(low, turned[z], tiles[z + 1]) for z in (0, 2)]
            at = pl.multiple_of(head * 128 + xy * 16, 16)
            for seq, value in ((0, first), (1, second)):
                aligned_ref[upper * 2 + seq, pl.ds(at, 16), :] = jnp.concatenate(
                    value, 0
                ).astype(BF16)
        return 0

    lax.fori_loop(0, back_ref.shape[0] // 4, arrange, 0)


def early_kernel(
    place_ref,
    left_ref,
    bias_ref,
    inverse_ref,
    compact_ref,
    z0_ref,
    z1_ref,
    z2_ref,
    x0_ref,
    x1_ref,
    x2_ref,
    part_ref,
    mid_ref,
    weight_ref,
):
    rows = left_ref.shape[0] // CO
    inner = z0_ref.shape[2] // CO

    def store(n, place, k, value):
        at = (n * inner + k) * rows
        part_ref[at : at + rows, :] = value

    project(EARLY, 3, (z0_ref, z1_ref, z2_ref), (x0_ref, x1_ref, x2_ref), left_ref, bias_ref,
            inverse_ref, compact_ref, place_ref, mid_ref, weight_ref, store)


def late_kernel(
    place_ref,
    left_ref,
    bias_ref,
    inverse_ref,
    compact_ref,
    part_ref,
    z0_ref,
    z1_ref,
    z2_ref,
    z3_ref,
    x0_ref,
    x1_ref,
    x2_ref,
    x3_ref,
    out_ref,
    mid_ref,
    weight_ref,
    turn_ref,
):
    rows = left_ref.shape[0] // CO
    inner = z0_ref.shape[2] // CO

    def store(n, place, k, value):
        at = pl.multiple_of((place * inner + k) * rows, rows)
        turn_ref[pl.ds(at, rows), :] = value

    project(LATE, 2, (z0_ref, z1_ref, z2_ref, z3_ref), (x0_ref, x1_ref, x2_ref, x3_ref),
            left_ref, bias_ref, inverse_ref, compact_ref, place_ref, mid_ref, weight_ref, store)
    block = inner * rows
    for n, (dz, dx, dy) in enumerate(EARLY):
        at = pl.multiple_of(place_ref[(dz * 4 + dx) * 2 + dy] * block, block)
        turn_ref[pl.ds(at, block), :] = part_ref[n * block : (n + 1) * block, :]
    columns = out_ref.shape[1]
    for i in range(rows):
        head = place_ref[len(EARLY) + len(LATE) + i // inner]
        out_ref[head * inner + i % inner] = turn_ref[pl.ds(i, columns, stride=rows), :]


def whole():
    return pl.BlockSpec(memory_space=pltpu.VMEM)


def per_device(
    msa,
    homolog,
    amino,
    gain,
    bias,
    focus,
    switch,
    final,
    final_bias,
    gain2,
    bias2,
    factors,
    pair_weight,
    pair_bias,
):
    n_dap, n_head = lax.axis_size("dap"), lax.axis_size("head")
    head_id, dap_id = lax.axis_index("head"), lax.axis_index("dap")
    own_seqs, residues, chans = msa.shape
    seqs = homolog.shape[0]
    width = focus.shape[2]
    col_width = residues // n_head
    mine = col_width // n_dap
    nz, nx, ny = 4, 4, 2

    parts = jnp.moveaxis(focus, 0, 2).reshape(4 * width, chans)
    first = lax.reduce_precision(switch, 8, 7)
    second = lax.reduce_precision(switch - first, 8, 7)
    third = switch - first - second
    offsets = jnp.zeros((16, chans), BF16)
    offsets = offsets.at[:3, :width].set(jnp.stack([first, second, third]).astype(BF16))
    bundle = jnp.concatenate([parts, final, offsets], 0)
    swap_core = [(h, h ^ 1) for h in range(n_head)]
    across = [
        (d * n_head + h, (d ^ 1) * n_head + (h ^ 2))
        for d in range(n_dap)
        for h in range(n_head)
    ]
    far_bundle = lax.ppermute(bundle, ("dap", "head"), across)
    bundles = [
        bundle,
        lax.ppermute(bundle, "head", swap_core),
        far_bundle,
        lax.ppermute(far_bundle, "head", swap_core),
    ]
    base = 5 * width
    shift = jnp.stack([b[base : base + 3, :width] for b in bundles]).astype(F32)
    shift = ((shift[:, 0] + shift[:, 1]) + shift[:, 2]).reshape(chans, 1)

    block = lax.dynamic_slice_in_dim(msa, head_id * col_width, col_width, 1)
    block = block.reshape(own_seqs, nx, ny, nz, mine, chans)
    block = block.transpose(3, 1, 2, 4, 0, 5).reshape(n_dap, mine * own_seqs, chans)
    block = lax.all_to_all(block, "dap", split_axis=0, concat_axis=0, tiled=True)

    keep = homolog.astype(F32)
    eye = jnp.eye(mine, dtype=BF16)
    right_weight = (eye[:, None, :, None] * factors[:, 1][None, :, None, :]).reshape(
        mine, chans, mine * CO
    )
    left_weight = factors[:, 0].T
    zi, xi, yi = dap_id // (nx * ny), (dap_id // ny) % nx, dap_id % ny
    start = head_id * col_width + xi * (ny * nz * mine) + yi * (nz * mine) + zi * mine
    own_amino = lax.dynamic_slice_in_dim(amino, start, mine)
    row = lambda v: v.reshape(1, chans)
    lanes = mine * CO
    depth = pair_weight.shape[1]
    rows, left, right = pl.pallas_call(
        attend_kernel,
        in_specs=[
            pl.BlockSpec(memory_space=pltpu.SMEM),
            whole(),
            *[whole()] * n_head,
            whole(),
            whole(),
            whole(),
            whole(),
            whole(),
            whole(),
            whole(),
            whole(),
            whole(),
            whole(),
        ],
        out_specs=[whole(), whole(), whole()],
        out_shape=[
            jax.ShapeDtypeStruct((seqs * mine, chans), BF16),
            jax.ShapeDtypeStruct((mine, CO, seqs), BF16),
            jax.ShapeDtypeStruct((2, seqs // 2, lanes), BF16),
        ],
        scratch_shapes=[
            pltpu.VMEM((chans, seqs), BF16),
            pltpu.VMEM((chans // DH, seqs, 128), BF16),
            pltpu.VMEM((chans, seqs), BF16),
            pltpu.VMEM((chans, seqs), F32),
            pltpu.VMEM((chans, seqs), BF16),
            pltpu.VMEM((chans // 128, seqs * mine, 128), F32),
            pltpu.VMEM((seqs, lanes), F32),
        ],
        compiler_params=pltpu.CompilerParams(
            vmem_limit_bytes=24 * 2**20
        ),
        cost_estimate=pl.CostEstimate(
            flops=16_000_000_000, bytes_accessed=4 * 2**20, transcendentals=9_000_000
        ),
        name="attend",
    )(
        own_amino,
        block,
        *bundles,
        shift,
        row(gain),
        row(bias),
        row(final_bias),
        row(gain2),
        row(bias2),
        keep.reshape(seqs, 1),
        keep.reshape(1, seqs),
        right_weight,
        left_weight,
    )

    swap = []
    for z in range(nz):
        for rest in range(nx * ny):
            for h in range(n_head):
                swap.append(
                    ((z * nx * ny + rest) * n_head + h, (h * nx * ny + rest) * n_head + z)
                )
    left = lax.ppermute(left, ("dap", "head"), swap)

    def shifted(value, axis, by):
        pairs = []
        for z in range(nz):
            for x in range(nx):
                for y in range(ny):
                    to = [z, x, y]
                    to[axis] = (to[axis] + by) % (nz, nx, ny)[axis]
                    pairs.append(((z * nx + x) * ny + y, (to[0] * nx + to[1]) * ny + to[2]))
        return lax.ppermute(value, "dap", pairs)

    other = shifted(right, 2, 1)

    def first_stage(value, axis):
        return [value] + [shifted(value, axis, -step) for step in STEPS[1:]]

    def second_stage(value, axis):
        from_left, from_right = shifted(value, axis, 1), shifted(value, axis, -1)
        return value, from_left, from_right

    colours = [jnp.stack([right[part], other[part]]) for part in range(2)]
    parts = first_stage(colours[0], 1) + first_stage(colours[1], 0)
    shape = (len(STEPS) * ny, *parts[0].shape[1:])
    mids = pl.pallas_call(
        join_kernel,
        in_specs=[pl.BlockSpec(memory_space=pltpu.VMEM)] * len(parts),
        out_specs=[pl.BlockSpec(memory_space=pltpu.VMEM)] * 2,
        out_shape=[jax.ShapeDtypeStruct(shape, BF16)] * 2,
        compiler_params=pltpu.CompilerParams(vmem_limit_bytes=4 * 2**20),
        cost_estimate=pl.CostEstimate(
            flops=2_000_000, bytes_accessed=2 * 2**20, transcendentals=0
        ),
        name="join",
    )(*parts)
    (*mids, left) = lax.optimization_barrier((*mids, left))
    z_pieces = second_stage(mids[0], 0)
    x_pieces = second_stage(mids[1], 1)
    z_pieces = (*z_pieces, shifted(z_pieces[1], 0, 1))
    x_pieces = (*x_pieces, shifted(x_pieces[1], 1, 1))

    left_core = lax.ppermute(left, "head", swap_core)
    left_far = lax.ppermute(left, "head", [(h, h ^ 2) for h in range(n_head)])
    left_corner = lax.ppermute(left_far, "head", swap_core)
    i_rows = mine * n_head
    left = jnp.concatenate([left, left_core, left_far, left_corner], 0)
    left = jnp.swapaxes(left, 0, 1).reshape(CO * i_rows, seqs)

    back = lax.all_to_all(
        rows.reshape(n_dap * n_head, seqs * mine // (n_dap * n_head), chans),
        ("dap", "head"),
        split_axis=0,
        concat_axis=0,
        tiled=True,
    )
    own = own_seqs // n_head
    total = jnp.sum(homolog).astype(F32)
    row_keep = lax.dynamic_slice_in_dim(amino, dap_id * i_rows, i_rows).astype(F32)
    heads = [head_id ^ flip for flip in range(n_head)]
    row_keep = jnp.concatenate(
        [lax.dynamic_slice_in_dim(row_keep, h * mine, mine) for h in heads]
    )
    col_keep = lax.dynamic_slice_in_dim(amino, head_id * col_width, col_width).astype(F32)
    norm = jnp.maximum(
        total * row_keep[None, :, None] * col_keep.reshape(n_dap, 1, mine), 1.0
    )
    inverse = (1.0 / norm).reshape(n_dap * i_rows, mine)
    places = []
    for dz in STEPS:
        for dx in STEPS:
            for dy in range(ny):
                at_z, at_x, at_y = (zi + dz) % nz, (xi + dx) % nx, (yi + dy) % ny
                places.append((at_x * ny + at_y) * nz + at_z)
    shared = (
        jnp.stack([*places, *heads]).astype(jnp.int32),
        left,
        pair_bias.reshape(1, depth),
        inverse,
        pair_weight,
    )
    early = pl.pallas_call(
        early_kernel,
        in_specs=[
            pl.BlockSpec(memory_space=pltpu.SMEM),
            *[pl.BlockSpec(memory_space=pltpu.VMEM)] * 10,
        ],
        out_specs=pl.BlockSpec(memory_space=pltpu.VMEM),
        out_shape=jax.ShapeDtypeStruct((len(EARLY) * mine * i_rows, depth), F32),
        scratch_shapes=[
            pltpu.VMEM((len(EARLY) * i_rows, CO * lanes), BF16),
            pltpu.VMEM((CO * lanes, mine * depth), BF16),
        ],
        compiler_params=pltpu.CompilerParams(vmem_limit_bytes=18 * 2**20),
        cost_estimate=pl.CostEstimate(
            flops=3_000_000_000, bytes_accessed=6 * 2**20, transcendentals=0
        ),
        name="early",
    )(*shared, *z_pieces[:3], *x_pieces[:3])
    alignment = pl.pallas_call(
        arrange_kernel,
        in_specs=[pl.BlockSpec(memory_space=pltpu.VMEM)],
        out_specs=pl.BlockSpec(memory_space=pltpu.VMEM),
        out_shape=jax.ShapeDtypeStruct((own, residues, chans), BF16),
        compiler_params=pltpu.CompilerParams(vmem_limit_bytes=8 * 2**20),
        cost_estimate=pl.CostEstimate(
            flops=500_000_000, bytes_accessed=2 * 2**20, transcendentals=0
        ),
        name="arrange",
    )(back)
    pair = pl.pallas_call(
        late_kernel,
        in_specs=[
            pl.BlockSpec(memory_space=pltpu.SMEM),
            *[pl.BlockSpec(memory_space=pltpu.VMEM)] * 13,
        ],
        out_specs=pl.BlockSpec(memory_space=pltpu.VMEM),
        out_shape=jax.ShapeDtypeStruct((i_rows, col_width, depth), F32),
        scratch_shapes=[
            pltpu.VMEM((len(LATE) * i_rows, CO * lanes), BF16),
            pltpu.VMEM((CO * lanes, mine * depth), BF16),
            pltpu.VMEM((col_width * i_rows, depth), F32),
        ],
        compiler_params=pltpu.CompilerParams(vmem_limit_bytes=18 * 2**20),
        cost_estimate=pl.CostEstimate(
            flops=3_000_000_000, bytes_accessed=6 * 2**20, transcendentals=0
        ),
        name="late",
    )(*shared, early, *z_pieces, *x_pieces)
    return alignment, pair


def solution(mesh):
    return jax.shard_map(
        per_device,
        mesh=mesh,
        in_specs=(
            P("dap", None, None),
            P(),
            P(),
            P(),
            P(),
            P(None, None, "head"),
            P("head"),
            P("head", None),
            P(),
            P(),
            P(),
            P(),
            P(),
            P(),
        ),
        out_specs=(P(("dap", "head"), None, None), P("dap", "head", None)),
        check_vma=False,
    )
```

```python
import math

import jax
import jax.numpy as jnp
import numpy as np
from jax import lax
from jax.experimental import pallas as pl
from jax.experimental.pallas import tpu as pltpu
from jax.sharding import PartitionSpec as P

DH = 32
CO = 32
STEPS = (0, -1, 1, 2)
LOG2E = math.log2(math.e)


def bf16_terms(value):
    terms = []
    for _ in range(3):
        term = float(np.float32(value).astype(jnp.bfloat16))
        terms.append(term)
        value = float(np.float32(value)) - term
    return tuple(terms)


MASKS = bf16_terms(-1e9 * LOG2E)
NT = (((1,), (1,)), ((), ()))
TN = (((0,), (0,)), ((), ()))
F32 = jnp.float32
BF16 = jnp.bfloat16


def layer_norm(value, gain, bias):
    mean = jnp.mean(value, -1, keepdims=True)
    centred = value - mean
    spread = jnp.mean(centred * centred, -1, keepdims=True)
    return centred * lax.rsqrt(spread + 1e-05) * gain + bias


def attend_kernel(
    amino_ref,
    x_ref,
    w0_ref,
    w1_ref,
    w2_ref,
    w3_ref,
    shift_ref,
    gain_ref,
    bias_ref,
    out_bias_ref,
    gain2_ref,
    bias2_ref,
    keep_col_ref,
    keep_row_ref,
    right_weight_ref,
    left_weight_ref,
    rows_ref,
    left_ref,
    right_ref,
    q_ref,
    k_ref,
    v_ref,
    g_ref,
    a_ref,
    rows_scratch,
    right_scratch,
):
    steps = left_ref.shape[0]
    seqs = keep_col_ref.shape[0]
    w_refs = (w0_ref, w1_ref, w2_ref, w3_ref)
    chans = w0_ref.shape[1]
    width = chans // len(w_refs)
    own = seqs // x_ref.shape[0]

    def weight(which):
        return jnp.concatenate([w[which * width : (which + 1) * width, :] for w in w_refs], 0)

    absent = 1.0 - keep_col_ref[...]
    column = lax.broadcasted_iota(jnp.int32, (seqs, 128), 1) - DH
    extra = jnp.where(column == 0, MASKS[0], jnp.where(column == 1, MASKS[1], MASKS[2]))
    extra = jnp.where((column >= 0) & (column < 3), extra * absent, 0.0).astype(BF16)
    for head in range(chans // DH):
        k_ref[head] = extra
    row = lax.broadcasted_iota(jnp.int32, (16, seqs), 0)
    rest = jnp.where(row < 3, 1.0, 0.0).astype(BF16)
    ones = jnp.ones((16, seqs), BF16)

    def body(step, _):
        at = pl.multiple_of(step * own, own)
        x = x_ref[:, pl.ds(at, own), :].reshape(seqs, chans).astype(F32)
        normed = layer_norm(x, gain_ref[...], bias_ref[...]).astype(BF16)

        def transposed(which):
            return lax.dot_general(weight(which), normed, NT, preferred_element_type=F32)

        q_ref[...] = (transposed(0) * (DH**-0.5 * LOG2E)).astype(BF16)
        keys = lax.dot_general(normed, weight(1), NT, preferred_element_type=F32)
        keys = (keys * keep_col_ref[...]).astype(BF16)
        for head in range(chans // DH):
            k_ref[head, :, :DH] = keys[:, head * DH : (head + 1) * DH]
        v_ref[...] = transposed(2).astype(BF16)
        g_ref[...] = jax.nn.sigmoid(transposed(3) + shift_ref[...])

        def score(index):
            head, part = index // 1, index % 1
            cols = slice(part * (seqs // 1), (part + 1) * (seqs // 1))
            query = jnp.concatenate([q_ref[head * DH : (head + 1) * DH, cols], rest[:, cols]], 0)
            return jnp.dot(k_ref[head, :, : DH + 16], query, preferred_element_type=F32)

        def soften(scores):
            top = jnp.max(scores, 0, keepdims=True)
            return jnp.exp2(scores - top).astype(BF16)

        def mix(index, probs):
            low, high = index * DH, (index + 1) * DH
            both = jnp.concatenate([v_ref[low:high, :], ones], 0)
            mixed = jnp.dot(both, probs, preferred_element_type=F32)
            scale = 1.0 / mixed[DH : DH + 1, :]
            a_ref[low:high, :] = (mixed[:DH, :] * scale * g_ref[low:high, :]).astype(BF16)

        count = chans // DH
        ahead, behind = score(0), None
        for index in range(count):
            now = ahead
            if index + 1 < count:
                ahead = score(index + 1)
            probs = soften(now)
            if behind is not None:
                mix(index - 1, behind)
            behind = probs
        mix(count - 1, behind)
        update = lax.dot_general(a_ref[...], weight(4), TN, preferred_element_type=F32)
        fresh = (x + update + out_bias_ref[...]).astype(BF16)
        wide = fresh.astype(F32)
        for part in range(chans // 128):
            rows_scratch[part, pl.ds(step, seqs, stride=steps), :] = wide[
                :, part * 128 : (part + 1) * 128
            ]
        opm = layer_norm(wide, gain2_ref[...], bias2_ref[...]).astype(BF16)
        here = amino_ref[step].astype(F32)
        left = lax.dot_general(left_weight_ref[...], opm, NT, preferred_element_type=F32)
        left_ref[step] = (left * (keep_row_ref[...] * here)).astype(BF16)
        right = jnp.dot(opm, right_weight_ref[step], preferred_element_type=F32)
        right_scratch[...] += right * (keep_col_ref[...] * here)
        return 0

    right_scratch[...] = jnp.zeros_like(right_scratch)
    lax.fori_loop(0, steps, body, 0, unroll=2)
    right_ref[...] = right_scratch[...].astype(BF16).reshape(right_ref.shape)
    for part in range(chans // 128):
        rows_ref[:, part * 128 : (part + 1) * 128] = rows_scratch[part].astype(BF16)


def join_kernel(*refs):
    half = (len(refs) - 2) // 2
    for colour in range(2):
        out_ref = refs[2 * half + colour]
        for index in range(half):
            piece = refs[colour * half + index]
            count = piece.shape[0]
            out_ref[index * count : (index + 1) * count] = piece[...]


def project(slots, groups, z_refs, x_refs, left_ref, bias_ref, inverse_ref, compact_ref,
            place_ref, mid_ref, weight_ref, store):
    lanes = z_refs[0].shape[2]
    depth = bias_ref.shape[1]
    inner = lanes // CO
    rows = left_ref.shape[0] // CO
    nothing = jnp.zeros((CO, depth), BF16)
    for c in range(CO):
        block = compact_ref[c * CO : (c + 1) * CO, :].astype(BF16)
        for k in range(inner):
            at = (c * inner + k) * CO
            for j in range(inner):
                weight_ref[at : at + CO, j * depth : (j + 1) * depth] = (
                    block if j == k else nothing
                )

    def source(dz, dx, dy):
        return jnp.concatenate([z_refs[dz][dx * 2 + dy], x_refs[dx][dz * 2 + dy]], 0)

    left = left_ref[...]
    size = len(slots) // groups
    for group in range(groups):
        batch = slots[group * size : (group + 1) * size]
        pieces = jnp.concatenate([source(*slot) for slot in batch], 1)
        outer = jnp.dot(left, pieces, preferred_element_type=F32).astype(BF16)
        for q in range(size):
            at = (group * size + q) * rows
            for c in range(CO):
                mid_ref[at : at + rows, c * lanes : (c + 1) * lanes] = outer[
                    c * rows : (c + 1) * rows, q * lanes : (q + 1) * lanes
                ]
    for k in range(0, inner, 2):
        total = jnp.dot(
            mid_ref[...],
            weight_ref[:, k * depth : (k + 2) * depth],
            preferred_element_type=F32,
        )
        for n, (dz, dx, dy) in enumerate(slots):
            place = place_ref[(dz * 4 + dx) * 2 + dy]
            inverse = inverse_ref[pl.ds(pl.multiple_of(place * rows, rows), rows), :]
            for j in range(2):
                value = total[n * rows : (n + 1) * rows, j * depth : (j + 1) * depth]
                value = (value + bias_ref[...]) * inverse[:, k + j : k + j + 1]
                store(n, place, k + j, value)


EARLY = tuple((dz, dx, dy) for dz in range(3) for dx in range(3) for dy in range(2))
LATE = tuple(
    (dz, dx, dy) for dz in range(4) for dx in range(4) for dy in range(2) if 3 in (dz, dx)
)


def arrange_kernel(back_ref, aligned_ref):
    low = lax.broadcasted_iota(jnp.int32, (8, back_ref.shape[2]), 0) < 4

    def arrange(index, _):
        head, xy = index // 8, index % 8
        blocks = [back_ref[(z * 8 + xy) * 4 + head].astype(F32) for z in range(4)]
        for upper in range(2):
            tiles = [b[upper * 8 : upper * 8 + 8] for b in blocks]
            turned = [pltpu.roll(t, 4, 0) for t in tiles]
            first = [jnp.where(low, tiles[z], turned[z + 1]) for z in (0, 2)]
            second = [jnp.where(low, turned[z], tiles[z + 1]) for z in (0, 2)]
            at = pl.multiple_of(head * 128 + xy * 16, 16)
            for seq, value in ((0, first), (1, second)):
                aligned_ref[upper * 2 + seq, pl.ds(at, 16), :] = jnp.concatenate(
                    value, 0
                ).astype(BF16)
        return 0

    lax.fori_loop(0, back_ref.shape[0] // 4, arrange, 0)


def early_kernel(
    place_ref,
    left_ref,
    bias_ref,
    inverse_ref,
    compact_ref,
    z0_ref,
    z1_ref,
    z2_ref,
    x0_ref,
    x1_ref,
    x2_ref,
    part_ref,
    mid_ref,
    weight_ref,
):
    rows = left_ref.shape[0] // CO
    inner = z0_ref.shape[2] // CO

    def store(n, place, k, value):
        at = (n * inner + k) * rows
        part_ref[at : at + rows, :] = value

    project(EARLY, 3, (z0_ref, z1_ref, z2_ref), (x0_ref, x1_ref, x2_ref), left_ref, bias_ref,
            inverse_ref, compact_ref, place_ref, mid_ref, weight_ref, store)


def late_kernel(
    place_ref,
    left_ref,
    bias_ref,
    inverse_ref,
    compact_ref,
    part_ref,
    z0_ref,
    z1_ref,
    z2_ref,
    z3_ref,
    x0_ref,
    x1_ref,
    x2_ref,
    x3_ref,
    out_ref,
    mid_ref,
    weight_ref,
    turn_ref,
):
    rows = left_ref.shape[0] // CO
    inner = z0_ref.shape[2] // CO

    def store(n, place, k, value):
        at = pl.multiple_of((place * inner + k) * rows, rows)
        turn_ref[pl.ds(at, rows), :] = value

    project(LATE, 2, (z0_ref, z1_ref, z2_ref, z3_ref), (x0_ref, x1_ref, x2_ref, x3_ref),
            left_ref, bias_ref, inverse_ref, compact_ref, place_ref, mid_ref, weight_ref, store)
    block = inner * rows
    for n, (dz, dx, dy) in enumerate(EARLY):
        at = pl.multiple_of(place_ref[(dz * 4 + dx) * 2 + dy] * block, block)
        turn_ref[pl.ds(at, block), :] = part_ref[n * block : (n + 1) * block, :]
    columns = out_ref.shape[1]
    for i in range(rows):
        head = place_ref[len(EARLY) + len(LATE) + i // inner]
        out_ref[head * inner + i % inner] = turn_ref[pl.ds(i, columns, stride=rows), :]


def whole():
    return pl.BlockSpec(memory_space=pltpu.VMEM)


def per_device(
    msa,
    homolog,
    amino,
    gain,
    bias,
    focus,
    switch,
    final,
    final_bias,
    gain2,
    bias2,
    factors,
    pair_weight,
    pair_bias,
):
    n_dap, n_head = lax.axis_size("dap"), lax.axis_size("head")
    head_id, dap_id = lax.axis_index("head"), lax.axis_index("dap")
    own_seqs, residues, chans = msa.shape
    seqs = homolog.shape[0]
    width = focus.shape[2]
    col_width = residues // n_head
    mine = col_width // n_dap
    nz, nx, ny = 4, 4, 2

    parts = jnp.moveaxis(focus, 0, 2).reshape(4 * width, chans)
    first = lax.reduce_precision(switch, 8, 7)
    second = lax.reduce_precision(switch - first, 8, 7)
    third = switch - first - second
    offsets = jnp.zeros((16, chans), BF16)
    offsets = offsets.at[:3, :width].set(jnp.stack([first, second, third]).astype(BF16))
    bundle = jnp.concatenate([parts, final, offsets], 0)
    swap_core = [(h, h ^ 1) for h in range(n_head)]
    across = [
        (d * n_head + h, (d ^ 1) * n_head + (h ^ 2))
        for d in range(n_dap)
        for h in range(n_head)
    ]
    far_bundle = lax.ppermute(bundle, ("dap", "head"), across)
    bundles = [
        bundle,
        lax.ppermute(bundle, "head", swap_core),
        far_bundle,
        lax.ppermute(far_bundle, "head", swap_core),
    ]
    base = 5 * width
    shift = jnp.stack([b[base : base + 3, :width] for b in bundles]).astype(F32)
    shift = ((shift[:, 0] + shift[:, 1]) + shift[:, 2]).reshape(chans, 1)

    block = lax.dynamic_slice_in_dim(msa, head_id * col_width, col_width, 1)
    block = block.reshape(own_seqs, nx, ny, nz, mine, chans)
    block = block.transpose(3, 1, 2, 4, 0, 5).reshape(n_dap, mine * own_seqs, chans)
    block = lax.all_to_all(block, "dap", split_axis=0, concat_axis=0, tiled=True)

    keep = homolog.astype(F32)
    eye = jnp.eye(mine, dtype=BF16)
    right_weight = (eye[:, None, :, None] * factors[:, 1][None, :, None, :]).reshape(
        mine, chans, mine * CO
    )
    left_weight = factors[:, 0].T
    zi, xi, yi = dap_id // (nx * ny), (dap_id // ny) % nx, dap_id % ny
    start = head_id * col_width + xi * (ny * nz * mine) + yi * (nz * mine) + zi * mine
    own_amino = lax.dynamic_slice_in_dim(amino, start, mine)
    row = lambda v: v.reshape(1, chans)
    lanes = mine * CO
    depth = pair_weight.shape[1]
    rows, left, right = pl.pallas_call(
        attend_kernel,
        in_specs=[
            pl.BlockSpec(memory_space=pltpu.SMEM),
            whole(),
            *[whole()] * n_head,
            whole(),
            whole(),
            whole(),
            whole(),
            whole(),
            whole(),
            whole(),
            whole(),
            whole(),
            whole(),
        ],
        out_specs=[whole(), whole(), whole()],
        out_shape=[
            jax.ShapeDtypeStruct((seqs * mine, chans), BF16),
            jax.ShapeDtypeStruct((mine, CO, seqs), BF16),
            jax.ShapeDtypeStruct((2, seqs // 2, lanes), BF16),
        ],
        scratch_shapes=[
            pltpu.VMEM((chans, seqs), BF16),
            pltpu.VMEM((chans // DH, seqs, 128), BF16),
            pltpu.VMEM((chans, seqs), BF16),
            pltpu.VMEM((chans, seqs), F32),
            pltpu.VMEM((chans, seqs), BF16),
            pltpu.VMEM((chans // 128, seqs * mine, 128), F32),
            pltpu.VMEM((seqs, lanes), F32),
        ],
        compiler_params=pltpu.CompilerParams(
            vmem_limit_bytes=24 * 2**20
        ),
        cost_estimate=pl.CostEstimate(
            flops=16_000_000_000, bytes_accessed=4 * 2**20, transcendentals=9_000_000
        ),
        name="attend",
    )(
        own_amino,
        block,
        *bundles,
        shift,
        row(gain),
        row(bias),
        row(final_bias),
        row(gain2),
        row(bias2),
        keep.reshape(seqs, 1),
        keep.reshape(1, seqs),
        right_weight,
        left_weight,
    )

    swap = []
    for z in range(nz):
        for rest in range(nx * ny):
            for h in range(n_head):
                swap.append(
                    ((z * nx * ny + rest) * n_head + h, (h * nx * ny + rest) * n_head + z)
                )
    left = lax.ppermute(left, ("dap", "head"), swap)

    def shifted(value, axis, by):
        pairs = []
        for z in range(nz):
            for x in range(nx):
                for y in range(ny):
                    to = [z, x, y]
                    to[axis] = (to[axis] + by) % (nz, nx, ny)[axis]
                    pairs.append(((z * nx + x) * ny + y, (to[0] * nx + to[1]) * ny + to[2]))
        return lax.ppermute(value, "dap", pairs)

    other = shifted(right, 2, 1)

    def first_stage(value, axis):
        return [value] + [shifted(value, axis, -step) for step in STEPS[1:]]

    def second_stage(value, axis):
        from_left, from_right = shifted(value, axis, 1), shifted(value, axis, -1)
        return value, from_left, from_right

    colours = [jnp.stack([right[part], other[part]]) for part in range(2)]
    parts = first_stage(colours[0], 1) + first_stage(colours[1], 0)
    shape = (len(STEPS) * ny, *parts[0].shape[1:])
    mids = pl.pallas_call(
        join_kernel,
        in_specs=[pl.BlockSpec(memory_space=pltpu.VMEM)] * len(parts),
        out_specs=[pl.BlockSpec(memory_space=pltpu.VMEM)] * 2,
        out_shape=[jax.ShapeDtypeStruct(shape, BF16)] * 2,
        compiler_params=pltpu.CompilerParams(vmem_limit_bytes=4 * 2**20),
        cost_estimate=pl.CostEstimate(
            flops=2_000_000, bytes_accessed=2 * 2**20, transcendentals=0
        ),
        name="join",
    )(*parts)
    left_core = lax.ppermute(left, "head", swap_core)
    left_far = lax.ppermute(left, "head", [(h, h ^ 2) for h in range(n_head)])
    left_corner = lax.ppermute(left_far, "head", swap_core)
    z_pieces = second_stage(mids[0], 0)
    x_pieces = second_stage(mids[1], 1)
    z_pieces = (*z_pieces, shifted(z_pieces[1], 0, 1))
    x_pieces = (*x_pieces, shifted(x_pieces[1], 1, 1))

    i_rows = mine * n_head
    left = jnp.concatenate([left, left_core, left_far, left_corner], 0)
    left = jnp.swapaxes(left, 0, 1).reshape(CO * i_rows, seqs)

    back = lax.all_to_all(
        rows.reshape(n_dap * n_head, seqs * mine // (n_dap * n_head), chans),
        ("dap", "head"),
        split_axis=0,
        concat_axis=0,
        tiled=True,
    )
    own = own_seqs // n_head
    total = jnp.sum(homolog).astype(F32)
    row_keep = lax.dynamic_slice_in_dim(amino, dap_id * i_rows, i_rows).astype(F32)
    heads = [head_id ^ flip for flip in range(n_head)]
    row_keep = jnp.concatenate(
        [lax.dynamic_slice_in_dim(row_keep, h * mine, mine) for h in heads]
    )
    col_keep = lax.dynamic_slice_in_dim(amino, head_id * col_width, col_width).astype(F32)
    norm = jnp.maximum(
        total * row_keep[None, :, None] * col_keep.reshape(n_dap, 1, mine), 1.0
    )
    inverse = (1.0 / norm).reshape(n_dap * i_rows, mine)
    places = []
    for dz in STEPS:
        for dx in STEPS:
            for dy in range(ny):
                at_z, at_x, at_y = (zi + dz) % nz, (xi + dx) % nx, (yi + dy) % ny
                places.append((at_x * ny + at_y) * nz + at_z)
    shared = (
        jnp.stack([*places, *heads]).astype(jnp.int32),
        left,
        pair_bias.reshape(1, depth),
        inverse,
        pair_weight,
    )
    early = pl.pallas_call(
        early_kernel,
        in_specs=[
            pl.BlockSpec(memory_space=pltpu.SMEM),
            *[pl.BlockSpec(memory_space=pltpu.VMEM)] * 10,
        ],
        out_specs=pl.BlockSpec(memory_space=pltpu.VMEM),
        out_shape=jax.ShapeDtypeStruct((len(EARLY) * mine * i_rows, depth), F32),
        scratch_shapes=[
            pltpu.VMEM((len(EARLY) * i_rows, CO * lanes), BF16),
            pltpu.VMEM((CO * lanes, mine * depth), BF16),
        ],
        compiler_params=pltpu.CompilerParams(vmem_limit_bytes=18 * 2**20),
        cost_estimate=pl.CostEstimate(
            flops=3_000_000_000, bytes_accessed=6 * 2**20, transcendentals=0
        ),
        name="early",
    )(*shared, *z_pieces[:3], *x_pieces[:3])
    alignment = pl.pallas_call(
        arrange_kernel,
        in_specs=[pl.BlockSpec(memory_space=pltpu.VMEM)],
        out_specs=pl.BlockSpec(memory_space=pltpu.VMEM),
        out_shape=jax.ShapeDtypeStruct((own, residues, chans), BF16),
        compiler_params=pltpu.CompilerParams(vmem_limit_bytes=8 * 2**20),
        cost_estimate=pl.CostEstimate(
            flops=500_000_000, bytes_accessed=2 * 2**20, transcendentals=0
        ),
        name="arrange",
    )(back)
    pair = pl.pallas_call(
        late_kernel,
        in_specs=[
            pl.BlockSpec(memory_space=pltpu.SMEM),
            *[pl.BlockSpec(memory_space=pltpu.VMEM)] * 13,
        ],
        out_specs=pl.BlockSpec(memory_space=pltpu.VMEM),
        out_shape=jax.ShapeDtypeStruct((i_rows, col_width, depth), F32),
        scratch_shapes=[
            pltpu.VMEM((len(LATE) * i_rows, CO * lanes), BF16),
            pltpu.VMEM((CO * lanes, mine * depth), BF16),
            pltpu.VMEM((col_width * i_rows, depth), F32),
        ],
        compiler_params=pltpu.CompilerParams(vmem_limit_bytes=18 * 2**20),
        cost_estimate=pl.CostEstimate(
            flops=3_000_000_000, bytes_accessed=6 * 2**20, transcendentals=0
        ),
        name="late",
    )(*shared, early, *z_pieces, *x_pieces)
    return alignment, pair


def solution(mesh):
    return jax.shard_map(
        per_device,
        mesh=mesh,
        in_specs=(
            P("dap", None, None),
            P(),
            P(),
            P(),
            P(),
            P(None, None, "head"),
            P("head"),
            P("head", None),
            P(),
            P(),
            P(),
            P(),
            P(),
            P(),
        ),
        out_specs=(P(("dap", "head"), None, None), P("dap", "head", None)),
        check_vma=False,
    )
```

```python
import math

import jax
import jax.numpy as jnp
import numpy as np
from jax import lax
from jax.experimental import pallas as pl
from jax.experimental.pallas import tpu as pltpu
from jax.sharding import PartitionSpec as P

DH = 32
CO = 32
STEPS = (0, -1, 1, 2)
LOG2E = math.log2(math.e)


def bf16_terms(value):
    terms = []
    for _ in range(3):
        term = float(np.float32(value).astype(jnp.bfloat16))
        terms.append(term)
        value = float(np.float32(value)) - term
    return tuple(terms)


MASKS = bf16_terms(-1e9 * LOG2E)
NT = (((1,), (1,)), ((), ()))
TN = (((0,), (0,)), ((), ()))
F32 = jnp.float32
BF16 = jnp.bfloat16


def layer_norm(value, gain, bias):
    mean = jnp.mean(value, -1, keepdims=True)
    centred = value - mean
    spread = jnp.mean(centred * centred, -1, keepdims=True)
    return centred * lax.rsqrt(spread + 1e-05) * gain + bias


def attend_kernel(
    amino_ref,
    x_ref,
    w0_ref,
    w1_ref,
    w2_ref,
    w3_ref,
    shift_ref,
    gain_ref,
    bias_ref,
    out_bias_ref,
    gain2_ref,
    bias2_ref,
    keep_col_ref,
    keep_row_ref,
    right_weight_ref,
    left_weight_ref,
    rows_ref,
    left_ref,
    right_ref,
    q_ref,
    k_ref,
    v_ref,
    g_ref,
    a_ref,
    rows_scratch,
    right_scratch,
):
    steps = left_ref.shape[0]
    seqs = keep_col_ref.shape[0]
    w_refs = (w0_ref, w1_ref, w2_ref, w3_ref)
    chans = w0_ref.shape[1]
    width = chans // len(w_refs)
    own = seqs // x_ref.shape[0]

    def weight(which):
        return jnp.concatenate([w[which * width : (which + 1) * width, :] for w in w_refs], 0)

    absent = 1.0 - keep_col_ref[...]
    column = lax.broadcasted_iota(jnp.int32, (seqs, 128), 1) - DH
    extra = jnp.where(column == 0, MASKS[0], jnp.where(column == 1, MASKS[1], MASKS[2]))
    extra = jnp.where((column >= 0) & (column < 3), extra * absent, 0.0).astype(BF16)
    for head in range(chans // DH):
        k_ref[head] = extra
    row = lax.broadcasted_iota(jnp.int32, (16, seqs), 0)
    rest = jnp.where(row < 3, 1.0, 0.0).astype(BF16)
    ones = jnp.ones((16, seqs), BF16)

    def body(step, _):
        at = pl.multiple_of(step * own, own)
        x = x_ref[:, pl.ds(at, own), :].reshape(seqs, chans).astype(F32)
        normed = layer_norm(x, gain_ref[...], bias_ref[...]).astype(BF16)

        def transposed(which):
            return lax.dot_general(weight(which), normed, NT, preferred_element_type=F32)

        q_ref[...] = (transposed(0) * (DH**-0.5 * LOG2E)).astype(BF16)
        keys = lax.dot_general(normed, weight(1), NT, preferred_element_type=F32)
        keys = (keys * keep_col_ref[...]).astype(BF16)
        for head in range(chans // DH):
            k_ref[head, :, :DH] = keys[:, head * DH : (head + 1) * DH]
        v_ref[...] = transposed(2).astype(BF16)
        g_ref[...] = jax.nn.sigmoid(transposed(3) + shift_ref[...])

        def score(index):
            head, part = index // 1, index % 1
            cols = slice(part * (seqs // 1), (part + 1) * (seqs // 1))
            query = jnp.concatenate([q_ref[head * DH : (head + 1) * DH, cols], rest[:, cols]], 0)
            return jnp.dot(k_ref[head, :, : DH + 16], query, preferred_element_type=F32)

        def soften(scores):
            top = jnp.max(scores, 0, keepdims=True)
            return jnp.exp2(scores - top).astype(BF16)

        def mix(index, probs):
            low, high = index * DH, (index + 1) * DH
            both = jnp.concatenate([v_ref[low:high, :], ones], 0)
            mixed = jnp.dot(both, probs, preferred_element_type=F32)
            scale = 1.0 / mixed[DH : DH + 1, :]
            a_ref[low:high, :] = (mixed[:DH, :] * scale * g_ref[low:high, :]).astype(BF16)

        count = chans // DH
        ahead, behind = score(0), None
        for index in range(count):
            now = ahead
            if index + 1 < count:
                ahead = score(index + 1)
            probs = soften(now)
            if behind is not None:
                mix(index - 1, behind)
            behind = probs
        mix(count - 1, behind)
        update = lax.dot_general(a_ref[...], weight(4), TN, preferred_element_type=F32)
        fresh = (x + update + out_bias_ref[...]).astype(BF16)
        wide = fresh.astype(F32)
        for part in range(chans // 128):
            rows_scratch[part, pl.ds(step, seqs, stride=steps), :] = wide[
                :, part * 128 : (part + 1) * 128
            ]
        opm = layer_norm(wide, gain2_ref[...], bias2_ref[...]).astype(BF16)
        here = amino_ref[step].astype(F32)
        left = lax.dot_general(left_weight_ref[...], opm, NT, preferred_element_type=F32)
        left_ref[step] = (left * (keep_row_ref[...] * here)).astype(BF16)
        right = jnp.dot(opm, right_weight_ref[step], preferred_element_type=F32)
        right_scratch[...] += right * (keep_col_ref[...] * here)
        return 0

    right_scratch[...] = jnp.zeros_like(right_scratch)
    lax.fori_loop(0, steps, body, 0, unroll=2)
    right_ref[...] = right_scratch[...].astype(BF16).reshape(right_ref.shape)
    for part in range(chans // 128):
        rows_ref[:, part * 128 : (part + 1) * 128] = rows_scratch[part].astype(BF16)


def join_kernel(*refs):
    half = (len(refs) - 2) // 2
    for colour in range(2):
        out_ref = refs[2 * half + colour]
        for index in range(half):
            piece = refs[colour * half + index]
            count = piece.shape[0]
            out_ref[index * count : (index + 1) * count] = piece[...]


def project(slots, groups, z_refs, x_refs, left_ref, bias_ref, inverse_ref, compact_ref,
            place_ref, mid_ref, weight_ref, store, lanes):
    depth = bias_ref.shape[1]
    inner = lanes // CO
    rows = left_ref.shape[0] // CO
    nothing = jnp.zeros((CO, depth), BF16)
    for c in range(CO):
        block = compact_ref[c * CO : (c + 1) * CO, :].astype(BF16)
        for k in range(inner):
            at = (c * inner + k) * CO
            for j in range(inner):
                weight_ref[at : at + CO, j * depth : (j + 1) * depth] = (
                    block if j == k else nothing
                )

    def source(dz, dx, dy):
        return jnp.concatenate([z_refs[dz][dx * 2 + dy], x_refs[dx][dz * 2 + dy]], 0)

    left = left_ref[...]
    size = len(slots) // groups
    for group in range(groups):
        batch = slots[group * size : (group + 1) * size]
        pieces = jnp.concatenate([source(*slot) for slot in batch], 1)
        outer = jnp.dot(left, pieces, preferred_element_type=F32).astype(BF16)
        for q in range(size):
            at = (group * size + q) * rows
            for c in range(CO):
                mid_ref[at : at + rows, c * lanes : (c + 1) * lanes] = outer[
                    c * rows : (c + 1) * rows, q * lanes : (q + 1) * lanes
                ]
    for k in range(0, inner, 2):
        total = jnp.dot(
            mid_ref[...],
            weight_ref[:, k * depth : (k + 2) * depth],
            preferred_element_type=F32,
        )
        for n, (dz, dx, dy) in enumerate(slots):
            place = place_ref[(dz * 4 + dx) * 2 + dy]
            inverse = inverse_ref[pl.ds(pl.multiple_of(place * rows, rows), rows), :]
            for j in range(2):
                value = total[n * rows : (n + 1) * rows, j * depth : (j + 1) * depth]
                value = (value + bias_ref[...]) * inverse[:, k + j : k + j + 1]
                store(n, place, k + j, value)


EARLY = tuple((dz, dx, dy) for dz in range(3) for dx in range(3) for dy in range(2))
LATE = tuple(
    (dz, dx, dy) for dz in range(4) for dx in range(4) for dy in range(2) if 3 in (dz, dx)
)


def arrange_kernel(back_ref, aligned_ref):
    low = lax.broadcasted_iota(jnp.int32, (8, back_ref.shape[2]), 0) < 4

    def arrange(index, _):
        head, xy = index // 8, index % 8
        blocks = [back_ref[(z * 8 + xy) * 4 + head].astype(F32) for z in range(4)]
        for upper in range(2):
            tiles = [b[upper * 8 : upper * 8 + 8] for b in blocks]
            turned = [pltpu.roll(t, 4, 0) for t in tiles]
            first = [jnp.where(low, tiles[z], turned[z + 1]) for z in (0, 2)]
            second = [jnp.where(low, turned[z], tiles[z + 1]) for z in (0, 2)]
            at = pl.multiple_of(head * 128 + xy * 16, 16)
            for seq, value in ((0, first), (1, second)):
                aligned_ref[upper * 2 + seq, pl.ds(at, 16), :] = jnp.concatenate(
                    value, 0
                ).astype(BF16)
        return 0

    lax.fori_loop(0, back_ref.shape[0] // 4, arrange, 0)


def early_kernel(
    place_ref,
    left_ref,
    bias_ref,
    inverse_ref,
    compact_ref,
    z0_ref,
    z1_ref,
    z2_ref,
    x0_ref,
    x1_ref,
    x2_ref,
    part_ref,
    mid_ref,
    weight_ref,
):
    rows = left_ref.shape[0] // CO
    inner = z0_ref.shape[2] // CO

    def store(n, place, k, value):
        at = (n * inner + k) * rows
        part_ref[at : at + rows, :] = value

    project(EARLY, 3, (z0_ref, z1_ref, z2_ref), (x0_ref, x1_ref, x2_ref), left_ref, bias_ref,
            inverse_ref, compact_ref, place_ref, mid_ref, weight_ref, store,
            lanes=z0_ref.shape[2])


class Tail:
    def __init__(self, first, *refs):
        self.first, self.refs = first, refs

    def __getitem__(self, index):
        index -= self.first
        count = self.refs[0].shape[0]
        return self.refs[index // count][index % count]


def late_kernel(
    place_ref,
    left_ref,
    bias_ref,
    inverse_ref,
    compact_ref,
    part_ref,
    z0_ref,
    z1_ref,
    z2_ref,
    za_ref,
    zb_ref,
    x0_ref,
    x1_ref,
    x2_ref,
    xa_ref,
    xb_ref,
    out_ref,
    mid_ref,
    weight_ref,
    turn_ref,
):
    first = 3 * z0_ref.shape[0]
    z_refs = (*[Tail(first, ref) for ref in (z0_ref, z1_ref, z2_ref)], Tail(0, za_ref, zb_ref))
    x_refs = (*[Tail(first, ref) for ref in (x0_ref, x1_ref, x2_ref)], Tail(0, xa_ref, xb_ref))
    rows = left_ref.shape[0] // CO
    inner = z0_ref.shape[2] // CO

    def store(n, place, k, value):
        at = pl.multiple_of((place * inner + k) * rows, rows)
        turn_ref[pl.ds(at, rows), :] = value

    project(LATE, 2, z_refs, x_refs, left_ref, bias_ref, inverse_ref, compact_ref, place_ref,
            mid_ref, weight_ref, store, lanes=z0_ref.shape[2])
    block = inner * rows
    for n, (dz, dx, dy) in enumerate(EARLY):
        at = pl.multiple_of(place_ref[(dz * 4 + dx) * 2 + dy] * block, block)
        turn_ref[pl.ds(at, block), :] = part_ref[n * block : (n + 1) * block, :]
    columns = out_ref.shape[1]
    for i in range(rows):
        head = place_ref[len(EARLY) + len(LATE) + i // inner]
        out_ref[head * inner + i % inner] = turn_ref[pl.ds(i, columns, stride=rows), :]


def whole(shape):
    return pl.BlockSpec(memory_space=pltpu.VMEM)


def per_device(
    msa,
    homolog,
    amino,
    gain,
    bias,
    focus,
    switch,
    final,
    final_bias,
    gain2,
    bias2,
    factors,
    pair_weight,
    pair_bias,
):
    n_dap, n_head = lax.axis_size("dap"), lax.axis_size("head")
    head_id, dap_id = lax.axis_index("head"), lax.axis_index("dap")
    own_seqs, residues, chans = msa.shape
    seqs = homolog.shape[0]
    width = focus.shape[2]
    col_width = residues // n_head
    mine = col_width // n_dap
    nz, nx, ny = 4, 4, 2

    parts = jnp.moveaxis(focus, 0, 2).reshape(4 * width, chans)
    first = lax.reduce_precision(switch, 8, 7)
    second = lax.reduce_precision(switch - first, 8, 7)
    third = switch - first - second
    offsets = jnp.zeros((16, chans), BF16)
    offsets = offsets.at[:3, :width].set(jnp.stack([first, second, third]).astype(BF16))
    bundle = jnp.concatenate([parts, final, offsets], 0)
    swap_core = [(h, h ^ 1) for h in range(n_head)]
    across = [
        (d * n_head + h, (d ^ 1) * n_head + (h ^ 2))
        for d in range(n_dap)
        for h in range(n_head)
    ]
    far_bundle = lax.ppermute(bundle, ("dap", "head"), across)
    bundles = [
        bundle,
        lax.ppermute(bundle, "head", swap_core),
        far_bundle,
        lax.ppermute(far_bundle, "head", swap_core),
    ]
    base = 5 * width
    shift = jnp.stack([b[base : base + 3, :width] for b in bundles]).astype(F32)
    shift = ((shift[:, 0] + shift[:, 1]) + shift[:, 2]).reshape(chans, 1)

    block = lax.dynamic_slice_in_dim(msa, head_id * col_width, col_width, 1)
    block = block.reshape(own_seqs, nx, ny, nz, mine, chans)
    block = block.transpose(3, 1, 2, 4, 0, 5).reshape(n_dap, mine * own_seqs, chans)
    block = lax.all_to_all(block, "dap", split_axis=0, concat_axis=0, tiled=True)

    keep = homolog.astype(F32)
    eye = jnp.eye(mine, dtype=BF16)
    right_weight = (eye[:, None, :, None] * factors[:, 1][None, :, None, :]).reshape(
        mine, chans, mine * CO
    )
    left_weight = factors[:, 0].T
    zi, xi, yi = dap_id // (nx * ny), (dap_id // ny) % nx, dap_id % ny
    start = head_id * col_width + xi * (ny * nz * mine) + yi * (nz * mine) + zi * mine
    own_amino = lax.dynamic_slice_in_dim(amino, start, mine)
    row = lambda v: v.reshape(1, chans)
    lanes = mine * CO
    depth = pair_weight.shape[1]
    rows, left, right = pl.pallas_call(
        attend_kernel,
        in_specs=[
            pl.BlockSpec(memory_space=pltpu.SMEM),
            whole(block.shape),
            *[whole(bundle.shape)] * n_head,
            whole((chans, 1)),
            whole((1, chans)),
            whole((1, chans)),
            whole((1, chans)),
            whole((1, chans)),
            whole((1, chans)),
            whole((seqs, 1)),
            whole((1, seqs)),
            whole((mine, chans, lanes)),
            whole((CO, chans)),
        ],
        out_specs=[
            whole((seqs * mine, chans)),
            whole((mine, CO, seqs)),
            whole((2, seqs // 2, lanes)),
        ],
        out_shape=[
            jax.ShapeDtypeStruct((seqs * mine, chans), BF16),
            jax.ShapeDtypeStruct((mine, CO, seqs), BF16),
            jax.ShapeDtypeStruct((2, seqs // 2, lanes), BF16),
        ],
        scratch_shapes=[
            pltpu.VMEM((chans, seqs), BF16),
            pltpu.VMEM((chans // DH, seqs, 128), BF16),
            pltpu.VMEM((chans, seqs), BF16),
            pltpu.VMEM((chans, seqs), F32),
            pltpu.VMEM((chans, seqs), BF16),
            pltpu.VMEM((chans // 128, seqs * mine, 128), F32),
            pltpu.VMEM((seqs, lanes), F32),
        ],
        compiler_params=pltpu.CompilerParams(
            vmem_limit_bytes=24 * 2**20
        ),
        cost_estimate=pl.CostEstimate(
            flops=16_000_000_000, bytes_accessed=4 * 2**20, transcendentals=9_000_000
        ),
        name="attend",
    )(
        own_amino,
        block,
        *bundles,
        shift,
        row(gain),
        row(bias),
        row(final_bias),
        row(gain2),
        row(bias2),
        keep.reshape(seqs, 1),
        keep.reshape(1, seqs),
        right_weight,
        left_weight,
    )

    swap = []
    for z in range(nz):
        for rest in range(nx * ny):
            for h in range(n_head):
                swap.append(
                    ((z * nx * ny + rest) * n_head + h, (h * nx * ny + rest) * n_head + z)
                )
    left = lax.ppermute(left, ("dap", "head"), swap)

    def shifted(value, axis, by):
        pairs = []
        for z in range(nz):
            for x in range(nx):
                for y in range(ny):
                    to = [z, x, y]
                    to[axis] = (to[axis] + by) % (nz, nx, ny)[axis]
                    pairs.append(((z * nx + x) * ny + y, (to[0] * nx + to[1]) * ny + to[2]))
        return lax.ppermute(value, "dap", pairs)

    other = shifted(right, 2, 1)

    def first_stage(value, axis):
        return [value] + [shifted(value, axis, -step) for step in STEPS[1:]]

    def second_stage(value, axis):
        from_left, from_right = shifted(value, axis, 1), shifted(value, axis, -1)
        return value, from_left, from_right

    colours = [jnp.stack([right[part], other[part]]) for part in range(2)]
    parts = first_stage(colours[0], 1) + first_stage(colours[1], 0)
    shape = (len(STEPS) * ny, *parts[0].shape[1:])
    mids = pl.pallas_call(
        join_kernel,
        in_specs=[pl.BlockSpec(memory_space=pltpu.VMEM)] * len(parts),
        out_specs=[pl.BlockSpec(memory_space=pltpu.VMEM)] * 2,
        out_shape=[jax.ShapeDtypeStruct(shape, BF16)] * 2,
        compiler_params=pltpu.CompilerParams(vmem_limit_bytes=4 * 2**20),
        cost_estimate=pl.CostEstimate(
            flops=2_000_000, bytes_accessed=2 * 2**20, transcendentals=0
        ),
        name="join",
    )(*parts)
    left_core = lax.ppermute(left, "head", swap_core)
    left_far = lax.ppermute(left, "head", [(h, h ^ 2) for h in range(n_head)])
    left_corner = lax.ppermute(left_far, "head", swap_core)
    z_pieces = second_stage(mids[0], 0)
    x_pieces = second_stage(mids[1], 1)
    half = len(STEPS) * ny // 2

    def forward(pieces, axis):
        return (*pieces, shifted(pieces[1][:half], axis, 1), shifted(pieces[2][half:], axis, -1))

    z_pieces = forward(z_pieces, 0)
    x_pieces = forward(x_pieces, 1)

    i_rows = mine * n_head
    left = jnp.concatenate([left, left_core, left_far, left_corner], 0)
    left = jnp.swapaxes(left, 0, 1).reshape(CO * i_rows, seqs)

    back = lax.all_to_all(
        rows.reshape(n_dap * n_head, seqs * mine // (n_dap * n_head), chans),
        ("dap", "head"),
        split_axis=0,
        concat_axis=0,
        tiled=True,
    )
    own = own_seqs // n_head
    total = jnp.sum(homolog).astype(F32)
    row_keep = lax.dynamic_slice_in_dim(amino, dap_id * i_rows, i_rows).astype(F32)
    heads = [head_id ^ flip for flip in range(n_head)]
    row_keep = jnp.concatenate(
        [lax.dynamic_slice_in_dim(row_keep, h * mine, mine) for h in heads]
    )
    col_keep = lax.dynamic_slice_in_dim(amino, head_id * col_width, col_width).astype(F32)
    norm = jnp.maximum(
        total * row_keep[None, :, None] * col_keep.reshape(n_dap, 1, mine), 1.0
    )
    inverse = (1.0 / norm).reshape(n_dap * i_rows, mine)
    places = []
    for dz in STEPS:
        for dx in STEPS:
            for dy in range(ny):
                at_z, at_x, at_y = (zi + dz) % nz, (xi + dx) % nx, (yi + dy) % ny
                places.append((at_x * ny + at_y) * nz + at_z)
    shared = (
        jnp.stack([*places, *heads]).astype(jnp.int32),
        left,
        pair_bias.reshape(1, depth),
        inverse,
        pair_weight,
    )
    early = pl.pallas_call(
        early_kernel,
        in_specs=[
            pl.BlockSpec(memory_space=pltpu.SMEM),
            *[pl.BlockSpec(memory_space=pltpu.VMEM)] * 10,
        ],
        out_specs=pl.BlockSpec(memory_space=pltpu.VMEM),
        out_shape=jax.ShapeDtypeStruct((len(EARLY) * mine * i_rows, depth), F32),
        scratch_shapes=[
            pltpu.VMEM((len(EARLY) * i_rows, CO * lanes), BF16),
            pltpu.VMEM((CO * lanes, mine * depth), BF16),
        ],
        compiler_params=pltpu.CompilerParams(vmem_limit_bytes=18 * 2**20),
        cost_estimate=pl.CostEstimate(
            flops=3_000_000_000, bytes_accessed=6 * 2**20, transcendentals=0
        ),
        name="early",
    )(*shared, *z_pieces[:3], *x_pieces[:3])
    alignment = pl.pallas_call(
        arrange_kernel,
        in_specs=[pl.BlockSpec(memory_space=pltpu.VMEM)],
        out_specs=pl.BlockSpec(memory_space=pltpu.VMEM),
        out_shape=jax.ShapeDtypeStruct((own, residues, chans), BF16),
        compiler_params=pltpu.CompilerParams(vmem_limit_bytes=8 * 2**20),
        cost_estimate=pl.CostEstimate(
            flops=500_000_000, bytes_accessed=2 * 2**20, transcendentals=0
        ),
        name="arrange",
    )(back)
    early, alignment = lax.optimization_barrier((early, alignment))
    part_specs = [
        pl.BlockSpec((ny, *z_pieces[0].shape[1:]), lambda _: (len(STEPS) - 1, 0, 0))
    ] * 3 + [pl.BlockSpec(memory_space=pltpu.VMEM)] * 2
    pair = pl.pallas_call(
        late_kernel,
        grid=(1,),
        in_specs=[
            pl.BlockSpec(memory_space=pltpu.SMEM),
            *[pl.BlockSpec(memory_space=pltpu.VMEM)] * 5,
            *part_specs,
            *part_specs,
        ],
        out_specs=pl.BlockSpec(memory_space=pltpu.VMEM),
        out_shape=jax.ShapeDtypeStruct((i_rows, col_width, depth), F32),
        scratch_shapes=[
            pltpu.VMEM((len(LATE) * i_rows, CO * lanes), BF16),
            pltpu.VMEM((CO * lanes, mine * depth), BF16),
            pltpu.VMEM((col_width * i_rows, depth), F32),
        ],
        compiler_params=pltpu.CompilerParams(vmem_limit_bytes=18 * 2**20),
        cost_estimate=pl.CostEstimate(
            flops=3_000_000_000, bytes_accessed=6 * 2**20, transcendentals=0
        ),
        name="late",
    )(*shared, early, *z_pieces, *x_pieces)
    return alignment, pair


def solution(mesh):
    return jax.shard_map(
        per_device,
        mesh=mesh,
        in_specs=(
            P("dap", None, None),
            P(),
            P(),
            P(),
            P(),
            P(None, None, "head"),
            P("head"),
            P("head", None),
            P(),
            P(),
            P(),
            P(),
            P(),
            P(),
        ),
        out_specs=(P(("dap", "head"), None, None), P("dap", "head", None)),
        check_vma=False,
    )
```

```python
import math

import jax
import jax.numpy as jnp
import numpy as np
from jax import lax
from jax.experimental import pallas as pl
from jax.experimental.pallas import tpu as pltpu
from jax.sharding import PartitionSpec as P

DH = 32
CO = 32
STEPS = (0, -1, 1, 2)
LOG2E = math.log2(math.e)


def bf16_terms(value):
    terms = []
    for _ in range(3):
        term = float(np.float32(value).astype(jnp.bfloat16))
        terms.append(term)
        value = float(np.float32(value)) - term
    return tuple(terms)


MASKS = bf16_terms(-1e9 * LOG2E)
NT = (((1,), (1,)), ((), ()))
TN = (((0,), (0,)), ((), ()))
F32 = jnp.float32
BF16 = jnp.bfloat16


def layer_norm(value, gain, bias):
    mean = jnp.mean(value, -1, keepdims=True)
    centred = value - mean
    spread = jnp.mean(centred * centred, -1, keepdims=True)
    return centred * lax.rsqrt(spread + 1e-05) * gain + bias


def attend_kernel(
    amino_ref,
    x_ref,
    w0_ref,
    w1_ref,
    w2_ref,
    w3_ref,
    shift_ref,
    gain_ref,
    bias_ref,
    out_bias_ref,
    gain2_ref,
    bias2_ref,
    keep_col_ref,
    keep_row_ref,
    right_weight_ref,
    left_weight_ref,
    rows_ref,
    left_ref,
    right_ref,
    q_ref,
    k_ref,
    v_ref,
    g_ref,
    a_ref,
    rows_scratch,
    right_scratch,
):
    steps = left_ref.shape[0]
    seqs = keep_col_ref.shape[0]
    w_refs = (w0_ref, w1_ref, w2_ref, w3_ref)
    chans = w0_ref.shape[1]
    width = chans // len(w_refs)
    own = seqs // x_ref.shape[0]

    def weight(which):
        return jnp.concatenate([w[which * width : (which + 1) * width, :] for w in w_refs], 0)

    absent = 1.0 - keep_col_ref[...]
    column = lax.broadcasted_iota(jnp.int32, (seqs, 128), 1) - DH
    extra = jnp.where(column == 0, MASKS[0], jnp.where(column == 1, MASKS[1], MASKS[2]))
    extra = jnp.where((column >= 0) & (column < 3), extra * absent, 0.0).astype(BF16)
    for head in range(chans // DH):
        k_ref[head] = extra
    row = lax.broadcasted_iota(jnp.int32, (16, seqs), 0)
    rest = jnp.where(row < 3, 1.0, 0.0).astype(BF16)
    ones = jnp.ones((16, seqs), BF16)

    def body(step, _):
        at = pl.multiple_of(step * own, own)
        x = x_ref[:, pl.ds(at, own), :].reshape(seqs, chans).astype(F32)
        normed = layer_norm(x, gain_ref[...], bias_ref[...]).astype(BF16)

        def transposed(which):
            return lax.dot_general(weight(which), normed, NT, preferred_element_type=F32)

        q_ref[...] = (transposed(0) * (DH**-0.5 * LOG2E)).astype(BF16)
        keys = lax.dot_general(normed, weight(1), NT, preferred_element_type=F32)
        keys = (keys * keep_col_ref[...]).astype(BF16)
        for head in range(chans // DH):
            k_ref[head, :, :DH] = keys[:, head * DH : (head + 1) * DH]
        v_ref[...] = transposed(2).astype(BF16)
        g_ref[...] = jax.nn.sigmoid(transposed(3) + shift_ref[...])

        def score(index):
            head, part = index // 1, index % 1
            cols = slice(part * (seqs // 1), (part + 1) * (seqs // 1))
            query = jnp.concatenate([q_ref[head * DH : (head + 1) * DH, cols], rest[:, cols]], 0)
            return jnp.dot(k_ref[head, :, : DH + 16], query, preferred_element_type=F32)

        def soften(scores):
            top = jnp.max(scores, 0, keepdims=True)
            return jnp.exp2(scores - top).astype(BF16)

        def mix(index, probs):
            low, high = index * DH, (index + 1) * DH
            both = jnp.concatenate([v_ref[low:high, :], ones], 0)
            mixed = jnp.dot(both, probs, preferred_element_type=F32)
            scale = 1.0 / mixed[DH : DH + 1, :]
            a_ref[low:high, :] = (mixed[:DH, :] * scale * g_ref[low:high, :]).astype(BF16)

        count = chans // DH
        ahead, behind = score(0), None
        for index in range(count):
            now = ahead
            if index + 1 < count:
                ahead = score(index + 1)
            probs = soften(now)
            if behind is not None:
                mix(index - 1, behind)
            behind = probs
        mix(count - 1, behind)
        update = lax.dot_general(a_ref[...], weight(4), TN, preferred_element_type=F32)
        fresh = (x + update + out_bias_ref[...]).astype(BF16)
        wide = fresh.astype(F32)
        for part in range(chans // 128):
            rows_scratch[part, pl.ds(step, seqs, stride=steps), :] = wide[
                :, part * 128 : (part + 1) * 128
            ]
        opm = layer_norm(wide, gain2_ref[...], bias2_ref[...]).astype(BF16)
        here = amino_ref[step].astype(F32)
        left = lax.dot_general(left_weight_ref[...], opm, NT, preferred_element_type=F32)
        left_ref[step] = (left * (keep_row_ref[...] * here)).astype(BF16)
        right = jnp.dot(opm, right_weight_ref[step], preferred_element_type=F32)
        right_scratch[...] += right * (keep_col_ref[...] * here)
        return 0

    right_scratch[...] = jnp.zeros_like(right_scratch)
    lax.fori_loop(0, steps, body, 0, unroll=2)
    right_ref[...] = right_scratch[...].astype(BF16).reshape(right_ref.shape)
    for part in range(chans // 128):
        rows_ref[:, part * 128 : (part + 1) * 128] = rows_scratch[part].astype(BF16)


def join_kernel(*refs):
    count = (len(refs) - 4) // 2
    for colour in range(2):
        outs = refs[2 * count + 2 * colour :]
        for index in range(count):
            piece = refs[colour * count + index]
            size = piece.shape[0]
            at = index * size
            out_ref = outs[at // outs[0].shape[0]]
            at %= outs[0].shape[0]
            out_ref[at : at + size] = piece[...]


def project(slots, groups, z_refs, x_refs, left_ref, bias_ref, inverse_ref, compact_ref,
            place_ref, mid_ref, weight_ref, store, lanes):
    depth = bias_ref.shape[1]
    inner = lanes // CO
    rows = left_ref.shape[0] // CO
    nothing = jnp.zeros((CO, depth), BF16)
    for c in range(CO):
        block = compact_ref[c * CO : (c + 1) * CO, :].astype(BF16)
        for k in range(inner):
            at = (c * inner + k) * CO
            for j in range(inner):
                weight_ref[at : at + CO, j * depth : (j + 1) * depth] = (
                    block if j == k else nothing
                )

    def source(dz, dx, dy):
        return jnp.concatenate([z_refs[dz][dx * 2 + dy], x_refs[dx][dz * 2 + dy]], 0)

    left = left_ref[...]
    size = len(slots) // groups
    for group in range(groups):
        batch = slots[group * size : (group + 1) * size]
        pieces = jnp.concatenate([source(*slot) for slot in batch], 1)
        outer = jnp.dot(left, pieces, preferred_element_type=F32).astype(BF16)
        for q in range(size):
            at = (group * size + q) * rows
            for c in range(CO):
                mid_ref[at : at + rows, c * lanes : (c + 1) * lanes] = outer[
                    c * rows : (c + 1) * rows, q * lanes : (q + 1) * lanes
                ]
    for k in range(0, inner, 2):
        total = jnp.dot(
            mid_ref[...],
            weight_ref[:, k * depth : (k + 2) * depth],
            preferred_element_type=F32,
        )
        for n, (dz, dx, dy) in enumerate(slots):
            place = place_ref[(dz * 4 + dx) * 2 + dy]
            inverse = inverse_ref[pl.ds(pl.multiple_of(place * rows, rows), rows), :]
            for j in range(2):
                value = total[n * rows : (n + 1) * rows, j * depth : (j + 1) * depth]
                value = (value + bias_ref[...]) * inverse[:, k + j : k + j + 1]
                store(n, place, k + j, value)


EARLY = tuple((dz, dx, dy) for dz in range(3) for dx in range(3) for dy in range(2))
LATE = tuple(
    (dz, dx, dy) for dz in range(4) for dx in range(4) for dy in range(2) if 3 in (dz, dx)
)


def arrange_kernel(back_ref, aligned_ref):
    low = lax.broadcasted_iota(jnp.int32, (8, back_ref.shape[2]), 0) < 4

    def arrange(index, _):
        head, xy = index // 8, index % 8
        blocks = [back_ref[(z * 8 + xy) * 4 + head].astype(F32) for z in range(4)]
        for upper in range(2):
            tiles = [b[upper * 8 : upper * 8 + 8] for b in blocks]
            turned = [pltpu.roll(t, 4, 0) for t in tiles]
            first = [jnp.where(low, tiles[z], turned[z + 1]) for z in (0, 2)]
            second = [jnp.where(low, turned[z], tiles[z + 1]) for z in (0, 2)]
            at = pl.multiple_of(head * 128 + xy * 16, 16)
            for seq, value in ((0, first), (1, second)):
                aligned_ref[upper * 2 + seq, pl.ds(at, 16), :] = jnp.concatenate(
                    value, 0
                ).astype(BF16)
        return 0

    lax.fori_loop(0, back_ref.shape[0] // 4, arrange, 0)


class Tail:
    def __init__(self, first, *refs):
        self.first, self.refs = first, refs

    def __getitem__(self, index):
        index -= self.first
        count = self.refs[0].shape[0]
        return self.refs[index // count][index % count]


def early_kernel(
    place_ref, left_ref, bias_ref, inverse_ref, compact_ref, *refs
):
    z_parts, x_parts, (part_ref, mid_ref, weight_ref) = refs[:6], refs[6:12], refs[12:]
    z_refs = [Tail(0, *z_parts[at : at + 2]) for at in (0, 2, 4)]
    x_refs = [Tail(0, *x_parts[at : at + 2]) for at in (0, 2, 4)]
    rows = left_ref.shape[0] // CO
    lanes = z_parts[0].shape[2]
    inner = lanes // CO

    def store(n, place, k, value):
        at = (n * inner + k) * rows
        part_ref[at : at + rows, :] = value

    project(EARLY, 3, z_refs, x_refs, left_ref, bias_ref, inverse_ref, compact_ref, place_ref,
            mid_ref, weight_ref, store, lanes)


def late_kernel(
    place_ref,
    left_ref,
    bias_ref,
    inverse_ref,
    compact_ref,
    part_ref,
    z0_ref,
    z1_ref,
    z2_ref,
    za_ref,
    zb_ref,
    x0_ref,
    x1_ref,
    x2_ref,
    xa_ref,
    xb_ref,
    out_ref,
    mid_ref,
    weight_ref,
    turn_ref,
):
    first = 3 * z0_ref.shape[0]
    z_refs = (*[Tail(first, ref) for ref in (z0_ref, z1_ref, z2_ref)], Tail(0, za_ref, zb_ref))
    x_refs = (*[Tail(first, ref) for ref in (x0_ref, x1_ref, x2_ref)], Tail(0, xa_ref, xb_ref))
    rows = left_ref.shape[0] // CO
    inner = z0_ref.shape[2] // CO

    def store(n, place, k, value):
        at = pl.multiple_of((place * inner + k) * rows, rows)
        turn_ref[pl.ds(at, rows), :] = value

    project(LATE, 2, z_refs, x_refs, left_ref, bias_ref, inverse_ref, compact_ref, place_ref,
            mid_ref, weight_ref, store, lanes=z0_ref.shape[2])
    block = inner * rows
    for n, (dz, dx, dy) in enumerate(EARLY):
        at = pl.multiple_of(place_ref[(dz * 4 + dx) * 2 + dy] * block, block)
        turn_ref[pl.ds(at, block), :] = part_ref[n * block : (n + 1) * block, :]
    columns = out_ref.shape[1]
    for i in range(rows):
        head = place_ref[len(EARLY) + len(LATE) + i // inner]
        out_ref[head * inner + i % inner] = turn_ref[pl.ds(i, columns, stride=rows), :]


def whole(shape):
    return pl.BlockSpec(memory_space=pltpu.VMEM)


def per_device(
    msa,
    homolog,
    amino,
    gain,
    bias,
    focus,
    switch,
    final,
    final_bias,
    gain2,
    bias2,
    factors,
    pair_weight,
    pair_bias,
):
    n_dap, n_head = lax.axis_size("dap"), lax.axis_size("head")
    head_id, dap_id = lax.axis_index("head"), lax.axis_index("dap")
    own_seqs, residues, chans = msa.shape
    seqs = homolog.shape[0]
    width = focus.shape[2]
    col_width = residues // n_head
    mine = col_width // n_dap
    nz, nx, ny = 4, 4, 2

    parts = jnp.moveaxis(focus, 0, 2).reshape(4 * width, chans)
    first = lax.reduce_precision(switch, 8, 7)
    second = lax.reduce_precision(switch - first, 8, 7)
    third = switch - first - second
    offsets = jnp.zeros((16, chans), BF16)
    offsets = offsets.at[:3, :width].set(jnp.stack([first, second, third]).astype(BF16))
    bundle = jnp.concatenate([parts, final, offsets], 0)
    swap_core = [(h, h ^ 1) for h in range(n_head)]
    across = [
        (d * n_head + h, (d ^ 1) * n_head + (h ^ 2))
        for d in range(n_dap)
        for h in range(n_head)
    ]
    far_bundle = lax.ppermute(bundle, ("dap", "head"), across)
    bundles = [
        bundle,
        lax.ppermute(bundle, "head", swap_core),
        far_bundle,
        lax.ppermute(far_bundle, "head", swap_core),
    ]
    base = 5 * width
    shift = jnp.stack([b[base : base + 3, :width] for b in bundles]).astype(F32)
    shift = ((shift[:, 0] + shift[:, 1]) + shift[:, 2]).reshape(chans, 1)

    block = lax.dynamic_slice_in_dim(msa, head_id * col_width, col_width, 1)
    block = block.reshape(own_seqs, nx, ny, nz, mine, chans)
    block = block.transpose(3, 1, 2, 4, 0, 5).reshape(n_dap, mine * own_seqs, chans)
    block = lax.all_to_all(block, "dap", split_axis=0, concat_axis=0, tiled=True)

    keep = homolog.astype(F32)
    eye = jnp.eye(mine, dtype=BF16)
    right_weight = (eye[:, None, :, None] * factors[:, 1][None, :, None, :]).reshape(
        mine, chans, mine * CO
    )
    left_weight = factors[:, 0].T
    zi, xi, yi = dap_id // (nx * ny), (dap_id // ny) % nx, dap_id % ny
    start = head_id * col_width + xi * (ny * nz * mine) + yi * (nz * mine) + zi * mine
    own_amino = lax.dynamic_slice_in_dim(amino, start, mine)
    row = lambda v: v.reshape(1, chans)
    lanes = mine * CO
    depth = pair_weight.shape[1]
    i_rows = mine * n_head
    total = jnp.sum(homolog).astype(F32)
    row_keep = lax.dynamic_slice_in_dim(amino, dap_id * i_rows, i_rows).astype(F32)
    heads = [head_id ^ flip for flip in range(n_head)]
    row_keep = jnp.concatenate(
        [lax.dynamic_slice_in_dim(row_keep, h * mine, mine) for h in heads]
    )
    col_keep = lax.dynamic_slice_in_dim(amino, head_id * col_width, col_width).astype(F32)
    norm = jnp.maximum(
        total * row_keep[None, :, None] * col_keep.reshape(n_dap, 1, mine), 1.0
    )
    inverse = (1.0 / norm).reshape(n_dap * i_rows, mine)
    places = []
    for dz in STEPS:
        for dx in STEPS:
            for dy in range(ny):
                at_z, at_x, at_y = (zi + dz) % nz, (xi + dx) % nx, (yi + dy) % ny
                places.append((at_x * ny + at_y) * nz + at_z)
    place = jnp.stack([*places, *heads]).astype(jnp.int32)
    block, inverse, place = lax.optimization_barrier((block, inverse, place))
    rows, left, right = pl.pallas_call(
        attend_kernel,
        in_specs=[
            pl.BlockSpec(memory_space=pltpu.SMEM),
            whole(block.shape),
            *[whole(bundle.shape)] * n_head,
            whole((chans, 1)),
            whole((1, chans)),
            whole((1, chans)),
            whole((1, chans)),
            whole((1, chans)),
            whole((1, chans)),
            whole((seqs, 1)),
            whole((1, seqs)),
            whole((mine, chans, lanes)),
            whole((CO, chans)),
        ],
        out_specs=[
            whole((seqs * mine, chans)),
            whole((mine, CO, seqs)),
            whole((2, seqs // 2, lanes)),
        ],
        out_shape=[
            jax.ShapeDtypeStruct((seqs * mine, chans), BF16),
            jax.ShapeDtypeStruct((mine, CO, seqs), BF16),
            jax.ShapeDtypeStruct((2, seqs // 2, lanes), BF16),
        ],
        scratch_shapes=[
            pltpu.VMEM((chans, seqs), BF16),
            pltpu.VMEM((chans // DH, seqs, 128), BF16),
            pltpu.VMEM((chans, seqs), BF16),
            pltpu.VMEM((chans, seqs), F32),
            pltpu.VMEM((chans, seqs), BF16),
            pltpu.VMEM((chans // 128, seqs * mine, 128), F32),
            pltpu.VMEM((seqs, lanes), F32),
        ],
        compiler_params=pltpu.CompilerParams(
            vmem_limit_bytes=24 * 2**20
        ),
        cost_estimate=pl.CostEstimate(
            flops=16_000_000_000, bytes_accessed=4 * 2**20, transcendentals=9_000_000
        ),
        name="attend",
    )(
        own_amino,
        block,
        *bundles,
        shift,
        row(gain),
        row(bias),
        row(final_bias),
        row(gain2),
        row(bias2),
        keep.reshape(seqs, 1),
        keep.reshape(1, seqs),
        right_weight,
        left_weight,
    )

    swap = []
    for z in range(nz):
        for rest in range(nx * ny):
            for h in range(n_head):
                swap.append(
                    ((z * nx * ny + rest) * n_head + h, (h * nx * ny + rest) * n_head + z)
                )
    left = lax.ppermute(left, ("dap", "head"), swap)

    def shifted(value, axis, by):
        pairs = []
        for z in range(nz):
            for x in range(nx):
                for y in range(ny):
                    to = [z, x, y]
                    to[axis] = (to[axis] + by) % (nz, nx, ny)[axis]
                    pairs.append(((z * nx + x) * ny + y, (to[0] * nx + to[1]) * ny + to[2]))
        return lax.ppermute(value, "dap", pairs)

    other = shifted(right, 2, 1)

    def first_stage(value, axis):
        return [value] + [shifted(value, axis, -step) for step in STEPS[1:]]

    colours = [jnp.stack([right[part], other[part]]) for part in range(2)]
    parts = first_stage(colours[0], 1) + first_stage(colours[1], 0)
    shape = (len(STEPS) * ny // 2, *parts[0].shape[1:])
    mids = pl.pallas_call(
        join_kernel,
        in_specs=[pl.BlockSpec(memory_space=pltpu.VMEM)] * len(parts),
        out_specs=[pl.BlockSpec(memory_space=pltpu.VMEM)] * 4,
        out_shape=[jax.ShapeDtypeStruct(shape, BF16)] * 4,
        compiler_params=pltpu.CompilerParams(vmem_limit_bytes=4 * 2**20),
        cost_estimate=pl.CostEstimate(
            flops=2_000_000, bytes_accessed=2 * 2**20, transcendentals=0
        ),
        name="join",
    )(*parts)
    left_core = lax.ppermute(left, "head", swap_core)
    left_far = lax.ppermute(left, "head", [(h, h ^ 2) for h in range(n_head)])
    left_corner = lax.ppermute(left_far, "head", swap_core)
    groups = [(mids[0], mids[1], 0), (mids[2], mids[3], 1)]
    onward = [
        (shifted(low, axis, 1), shifted(high, axis, -1)) for low, high, axis in groups
    ]
    ended = [
        (shifted(high, axis, 1), shifted(low, axis, -1)) for low, high, axis in groups
    ]
    tails = [
        (shifted(up, axis, 1), shifted(down, axis, -1))
        for (up, down), (_, _, axis) in zip(onward, groups)
    ]
    z_pieces, x_pieces = [
        (low, high, up, rest_up, rest_down, down, *tail)
        for (low, high, _), (up, down), (rest_up, rest_down), tail in zip(
            groups, onward, ended, tails
        )
    ]
    left = jnp.concatenate([left, left_core, left_far, left_corner], 0)
    left = jnp.swapaxes(left, 0, 1).reshape(CO * i_rows, seqs)

    back = lax.all_to_all(
        rows.reshape(n_dap * n_head, seqs * mine // (n_dap * n_head), chans),
        ("dap", "head"),
        split_axis=0,
        concat_axis=0,
        tiled=True,
    )
    own = own_seqs // n_head
    shared = (
        place,
        left,
        pair_bias.reshape(1, depth),
        inverse,
        pair_weight,
    )
    early = pl.pallas_call(
        early_kernel,
        in_specs=[
            pl.BlockSpec(memory_space=pltpu.SMEM),
            *[pl.BlockSpec(memory_space=pltpu.VMEM)] * 16,
        ],
        out_specs=pl.BlockSpec(memory_space=pltpu.VMEM),
        out_shape=jax.ShapeDtypeStruct((len(EARLY) * mine * i_rows, depth), F32),
        scratch_shapes=[
            pltpu.VMEM((len(EARLY) * i_rows, CO * lanes), BF16),
            pltpu.VMEM((CO * lanes, mine * depth), BF16),
        ],
        compiler_params=pltpu.CompilerParams(vmem_limit_bytes=18 * 2**20),
        cost_estimate=pl.CostEstimate(
            flops=3_000_000_000, bytes_accessed=6 * 2**20, transcendentals=0
        ),
        name="early",
    )(*shared, *z_pieces[:6], *x_pieces[:6])
    alignment = pl.pallas_call(
        arrange_kernel,
        in_specs=[pl.BlockSpec(memory_space=pltpu.VMEM)],
        out_specs=pl.BlockSpec(memory_space=pltpu.VMEM),
        out_shape=jax.ShapeDtypeStruct((own, residues, chans), BF16),
        compiler_params=pltpu.CompilerParams(vmem_limit_bytes=8 * 2**20),
        cost_estimate=pl.CostEstimate(
            flops=500_000_000, bytes_accessed=2 * 2**20, transcendentals=0
        ),
        name="arrange",
    )(back)
    part_specs = [
        pl.BlockSpec((ny, *z_pieces[0].shape[1:]), lambda _: (1, 0, 0))
    ] * 3 + [pl.BlockSpec(memory_space=pltpu.VMEM)] * 2
    pair = pl.pallas_call(
        late_kernel,
        grid=(1,),
        in_specs=[
            pl.BlockSpec(memory_space=pltpu.SMEM),
            *[pl.BlockSpec(memory_space=pltpu.VMEM)] * 5,
            *part_specs,
            *part_specs,
        ],
        out_specs=pl.BlockSpec(memory_space=pltpu.VMEM),
        out_shape=jax.ShapeDtypeStruct((i_rows, col_width, depth), F32),
        scratch_shapes=[
            pltpu.VMEM((len(LATE) * i_rows, CO * lanes), BF16),
            pltpu.VMEM((CO * lanes, mine * depth), BF16),
            pltpu.VMEM((col_width * i_rows, depth), F32),
        ],
        compiler_params=pltpu.CompilerParams(vmem_limit_bytes=18 * 2**20),
        cost_estimate=pl.CostEstimate(
            flops=3_000_000_000, bytes_accessed=6 * 2**20, transcendentals=0
        ),
        name="late",
    )(
        *shared,
        early,
        *[pieces[at] for pieces in (z_pieces, x_pieces) for at in (1, 3, 5, 6, 7)],
    )
    return alignment, pair


def solution(mesh):
    return jax.shard_map(
        per_device,
        mesh=mesh,
        in_specs=(
            P("dap", None, None),
            P(),
            P(),
            P(),
            P(),
            P(None, None, "head"),
            P("head"),
            P("head", None),
            P(),
            P(),
            P(),
            P(),
            P(),
            P(),
        ),
        out_specs=(P(("dap", "head"), None, None), P("dap", "head", None)),
        check_vma=False,
    )
```

```python
import math

import jax
import jax.numpy as jnp
import numpy as np
from jax import lax
from jax.experimental import pallas as pl
from jax.experimental.pallas import tpu as pltpu
from jax.sharding import PartitionSpec as P

DH = 32
CO = 32
STEPS = (0, -1, 1, 2)
LOG2E = math.log2(math.e)


def bf16_terms(value):
    terms = []
    for _ in range(3):
        term = float(np.float32(value).astype(jnp.bfloat16))
        terms.append(term)
        value = float(np.float32(value)) - term
    return tuple(terms)


MASKS = bf16_terms(-1e9 * LOG2E)
NT = (((1,), (1,)), ((), ()))
TN = (((0,), (0,)), ((), ()))
F32 = jnp.float32
BF16 = jnp.bfloat16


def layer_norm(value, gain, bias):
    mean = jnp.mean(value, -1, keepdims=True)
    centred = value - mean
    spread = jnp.mean(centred * centred, -1, keepdims=True)
    return centred * lax.rsqrt(spread + 1e-05) * gain + bias


def attend_kernel(
    amino_ref,
    x_ref,
    w0_ref,
    w1_ref,
    w2_ref,
    w3_ref,
    shift_ref,
    gain_ref,
    bias_ref,
    out_bias_ref,
    gain2_ref,
    bias2_ref,
    keep_col_ref,
    keep_row_ref,
    right_weight_ref,
    left_weight_ref,
    rows_ref,
    left_ref,
    right_ref,
    q_ref,
    k_ref,
    v_ref,
    g_ref,
    a_ref,
    rows_scratch,
    right_scratch,
):
    steps = left_ref.shape[0]
    seqs = keep_col_ref.shape[0]
    w_refs = (w0_ref, w1_ref, w2_ref, w3_ref)
    chans = w0_ref.shape[1]
    width = chans // len(w_refs)
    own = seqs // x_ref.shape[0]

    def weight(which):
        return jnp.concatenate([w[which * width : (which + 1) * width, :] for w in w_refs], 0)

    absent = 1.0 - keep_col_ref[...]
    column = lax.broadcasted_iota(jnp.int32, (seqs, 128), 1) - DH
    extra = jnp.where(column == 0, MASKS[0], jnp.where(column == 1, MASKS[1], MASKS[2]))
    extra = jnp.where((column >= 0) & (column < 3), extra * absent, 0.0).astype(BF16)
    for head in range(chans // DH):
        k_ref[head] = extra
    row = lax.broadcasted_iota(jnp.int32, (16, seqs), 0)
    rest = jnp.where(row < 3, 1.0, 0.0).astype(BF16)
    ones = jnp.ones((16, seqs), BF16)

    def body(step, _):
        at = pl.multiple_of(step * own, own)
        x = x_ref[:, pl.ds(at, own), :].reshape(seqs, chans).astype(F32)
        normed = layer_norm(x, gain_ref[...], bias_ref[...]).astype(BF16)

        def transposed(which):
            return lax.dot_general(weight(which), normed, NT, preferred_element_type=F32)

        q_ref[...] = (transposed(0) * (DH**-0.5 * LOG2E)).astype(BF16)
        keys = lax.dot_general(normed, weight(1), NT, preferred_element_type=F32)
        keys = (keys * keep_col_ref[...]).astype(BF16)
        for head in range(chans // DH):
            k_ref[head, :, :DH] = keys[:, head * DH : (head + 1) * DH]
        v_ref[...] = transposed(2).astype(BF16)
        g_ref[...] = jax.nn.sigmoid(transposed(3) + shift_ref[...])

        def score(index):
            head, part = index // 1, index % 1
            cols = slice(part * (seqs // 1), (part + 1) * (seqs // 1))
            query = jnp.concatenate([q_ref[head * DH : (head + 1) * DH, cols], rest[:, cols]], 0)
            return jnp.dot(k_ref[head, :, : DH + 16], query, preferred_element_type=F32)

        def soften(scores):
            top = jnp.max(scores, 0, keepdims=True)
            return jnp.exp2(scores - top).astype(BF16)

        def mix(index, probs):
            low, high = index * DH, (index + 1) * DH
            both = jnp.concatenate([v_ref[low:high, :], ones], 0)
            mixed = jnp.dot(both, probs, preferred_element_type=F32)
            scale = 1.0 / mixed[DH : DH + 1, :]
            a_ref[low:high, :] = (mixed[:DH, :] * scale * g_ref[low:high, :]).astype(BF16)

        count = chans // DH
        ahead, behind = score(0), None
        for index in range(count):
            now = ahead
            if index + 1 < count:
                ahead = score(index + 1)
            probs = soften(now)
            if behind is not None:
                mix(index - 1, behind)
            behind = probs
        mix(count - 1, behind)
        update = lax.dot_general(a_ref[...], weight(4), TN, preferred_element_type=F32)
        fresh = (x + update + out_bias_ref[...]).astype(BF16)
        wide = fresh.astype(F32)
        for part in range(chans // 128):
            rows_scratch[part, pl.ds(step, seqs, stride=steps), :] = wide[
                :, part * 128 : (part + 1) * 128
            ]
        opm = layer_norm(wide, gain2_ref[...], bias2_ref[...]).astype(BF16)
        here = amino_ref[step].astype(F32)
        left = lax.dot_general(left_weight_ref[...], opm, NT, preferred_element_type=F32)
        left_ref[step] = (left * (keep_row_ref[...] * here)).astype(BF16)
        right = jnp.dot(opm, right_weight_ref[step], preferred_element_type=F32)
        right_scratch[...] += right * (keep_col_ref[...] * here)
        return 0

    right_scratch[...] = jnp.zeros_like(right_scratch)
    lax.fori_loop(0, steps, body, 0, unroll=2)
    right_ref[...] = right_scratch[...].astype(BF16).reshape(right_ref.shape)
    for part in range(chans // 128):
        rows_ref[:, part * 128 : (part + 1) * 128] = rows_scratch[part].astype(BF16)


def join_kernel(*refs):
    half = (len(refs) - 2) // 2
    for colour in range(2):
        out_ref = refs[2 * half + colour]
        for index in range(half):
            piece = refs[colour * half + index]
            count = piece.shape[0]
            out_ref[index * count : (index + 1) * count] = piece[...]


def project(slots, groups, z_refs, x_refs, left_ref, bias_ref, inverse_ref, compact_ref,
            place_ref, mid_ref, weight_ref, store, lanes):
    depth = bias_ref.shape[1]
    inner = lanes // CO
    rows = left_ref.shape[0] // CO
    nothing = jnp.zeros((CO, depth), BF16)
    for c in range(CO):
        block = compact_ref[c * CO : (c + 1) * CO, :].astype(BF16)
        for k in range(inner):
            at = (c * inner + k) * CO
            for j in range(inner):
                weight_ref[at : at + CO, j * depth : (j + 1) * depth] = (
                    block if j == k else nothing
                )

    def source(dz, dx, dy):
        return jnp.concatenate([z_refs[dz][dx * 2 + dy], x_refs[dx][dz * 2 + dy]], 0)

    left = left_ref[...]
    size = len(slots) // groups
    for group in range(groups):
        batch = slots[group * size : (group + 1) * size]
        pieces = jnp.concatenate([source(*slot) for slot in batch], 1)
        outer = jnp.dot(left, pieces, preferred_element_type=F32).astype(BF16)
        for q in range(size):
            at = (group * size + q) * rows
            for c in range(CO):
                mid_ref[at : at + rows, c * lanes : (c + 1) * lanes] = outer[
                    c * rows : (c + 1) * rows, q * lanes : (q + 1) * lanes
                ]
    for k in range(0, inner, 2):
        total = jnp.dot(
            mid_ref[...],
            weight_ref[:, k * depth : (k + 2) * depth],
            preferred_element_type=F32,
        )
        for n, (dz, dx, dy) in enumerate(slots):
            place = place_ref[(dz * 4 + dx) * 2 + dy]
            inverse = inverse_ref[pl.ds(pl.multiple_of(place * rows, rows), rows), :]
            for j in range(2):
                value = total[n * rows : (n + 1) * rows, j * depth : (j + 1) * depth]
                value = (value + bias_ref[...]) * inverse[:, k + j : k + j + 1]
                store(n, place, k + j, value)


EARLY = tuple((dz, dx, dy) for dz in range(3) for dx in range(3) for dy in range(2))
LATE = tuple(
    (dz, dx, dy) for dz in range(4) for dx in range(4) for dy in range(2) if 3 in (dz, dx)
)


def arrange_kernel(back_ref, aligned_ref):
    low = lax.broadcasted_iota(jnp.int32, (8, back_ref.shape[2]), 0) < 4

    def arrange(index, _):
        head, xy = index // 8, index % 8
        blocks = [back_ref[(z * 8 + xy) * 4 + head].astype(F32) for z in range(4)]
        for upper in range(2):
            tiles = [b[upper * 8 : upper * 8 + 8] for b in blocks]
            turned = [pltpu.roll(t, 4, 0) for t in tiles]
            first = [jnp.where(low, tiles[z], turned[z + 1]) for z in (0, 2)]
            second = [jnp.where(low, turned[z], tiles[z + 1]) for z in (0, 2)]
            at = pl.multiple_of(head * 128 + xy * 16, 16)
            for seq, value in ((0, first), (1, second)):
                aligned_ref[upper * 2 + seq, pl.ds(at, 16), :] = jnp.concatenate(
                    value, 0
                ).astype(BF16)
        return 0

    lax.fori_loop(0, back_ref.shape[0] // 4, arrange, 0)


def early_kernel(
    place_ref,
    left_ref,
    bias_ref,
    inverse_ref,
    compact_ref,
    z0_ref,
    z1_ref,
    z2_ref,
    x0_ref,
    x1_ref,
    x2_ref,
    part_ref,
    mid_ref,
    weight_ref,
):
    rows = left_ref.shape[0] // CO
    inner = z0_ref.shape[2] // CO

    def store(n, place, k, value):
        at = (n * inner + k) * rows
        part_ref[at : at + rows, :] = value

    project(EARLY, 3, (z0_ref, z1_ref, z2_ref), (x0_ref, x1_ref, x2_ref), left_ref, bias_ref,
            inverse_ref, compact_ref, place_ref, mid_ref, weight_ref, store,
            lanes=z0_ref.shape[2])


class Tail:
    def __init__(self, first, *refs):
        self.first, self.refs = first, refs

    def __getitem__(self, index):
        index -= self.first
        count = self.refs[0].shape[0]
        return self.refs[index // count][index % count]


def late_kernel(
    place_ref,
    left_ref,
    bias_ref,
    inverse_ref,
    compact_ref,
    part_ref,
    z0_ref,
    z1_ref,
    z2_ref,
    za_ref,
    zb_ref,
    x0_ref,
    x1_ref,
    x2_ref,
    xa_ref,
    xb_ref,
    out_ref,
    mid_ref,
    weight_ref,
    turn_ref,
):
    first = 3 * z0_ref.shape[0]
    z_refs = (*[Tail(first, ref) for ref in (z0_ref, z1_ref, z2_ref)], Tail(0, za_ref, zb_ref))
    x_refs = (*[Tail(first, ref) for ref in (x0_ref, x1_ref, x2_ref)], Tail(0, xa_ref, xb_ref))
    rows = left_ref.shape[0] // CO
    inner = z0_ref.shape[2] // CO

    def store(n, place, k, value):
        at = pl.multiple_of((place * inner + k) * rows, rows)
        turn_ref[pl.ds(at, rows), :] = value

    project(LATE, 2, z_refs, x_refs, left_ref, bias_ref, inverse_ref, compact_ref, place_ref,
            mid_ref, weight_ref, store, lanes=z0_ref.shape[2])
    block = inner * rows
    for n, (dz, dx, dy) in enumerate(EARLY):
        at = pl.multiple_of(place_ref[(dz * 4 + dx) * 2 + dy] * block, block)
        turn_ref[pl.ds(at, block), :] = part_ref[n * block : (n + 1) * block, :]
    columns = out_ref.shape[1]
    for i in range(rows):
        head = place_ref[len(EARLY) + len(LATE) + i // inner]
        out_ref[head * inner + i % inner] = turn_ref[pl.ds(i, columns, stride=rows), :]


def whole(shape):
    return pl.BlockSpec(memory_space=pltpu.VMEM)


def per_device(
    msa,
    homolog,
    amino,
    gain,
    bias,
    focus,
    switch,
    final,
    final_bias,
    gain2,
    bias2,
    factors,
    pair_weight,
    pair_bias,
):
    n_dap, n_head = lax.axis_size("dap"), lax.axis_size("head")
    head_id, dap_id = lax.axis_index("head"), lax.axis_index("dap")
    own_seqs, residues, chans = msa.shape
    seqs = homolog.shape[0]
    width = focus.shape[2]
    col_width = residues // n_head
    mine = col_width // n_dap
    nz, nx, ny = 4, 4, 2

    parts = jnp.moveaxis(focus, 0, 2).reshape(4 * width, chans)
    first = lax.reduce_precision(switch, 8, 7)
    second = lax.reduce_precision(switch - first, 8, 7)
    third = switch - first - second
    offsets = jnp.zeros((16, chans), BF16)
    offsets = offsets.at[:3, :width].set(jnp.stack([first, second, third]).astype(BF16))
    bundle = jnp.concatenate([parts, final, offsets], 0)
    swap_core = [(h, h ^ 1) for h in range(n_head)]
    across = [
        (d * n_head + h, (d ^ 1) * n_head + (h ^ 2))
        for d in range(n_dap)
        for h in range(n_head)
    ]
    far_bundle = lax.ppermute(bundle, ("dap", "head"), across)
    bundles = [
        bundle,
        lax.ppermute(bundle, "head", swap_core),
        far_bundle,
        lax.ppermute(far_bundle, "head", swap_core),
    ]
    base = 5 * width
    shift = jnp.stack([b[base : base + 3, :width] for b in bundles]).astype(F32)
    shift = ((shift[:, 0] + shift[:, 1]) + shift[:, 2]).reshape(chans, 1)

    block = lax.dynamic_slice_in_dim(msa, head_id * col_width, col_width, 1)
    block = block.reshape(own_seqs, nx, ny, nz, mine, chans)
    block = block.transpose(3, 1, 2, 4, 0, 5).reshape(n_dap, mine * own_seqs, chans)
    block = lax.all_to_all(block, "dap", split_axis=0, concat_axis=0, tiled=True)

    keep = homolog.astype(F32)
    eye = jnp.eye(mine, dtype=BF16)
    right_weight = (eye[:, None, :, None] * factors[:, 1][None, :, None, :]).reshape(
        mine, chans, mine * CO
    )
    left_weight = factors[:, 0].T
    zi, xi, yi = dap_id // (nx * ny), (dap_id // ny) % nx, dap_id % ny
    start = head_id * col_width + xi * (ny * nz * mine) + yi * (nz * mine) + zi * mine
    own_amino = lax.dynamic_slice_in_dim(amino, start, mine)
    row = lambda v: v.reshape(1, chans)
    lanes = mine * CO
    depth = pair_weight.shape[1]
    i_rows = mine * n_head
    total = jnp.sum(homolog).astype(F32)
    row_keep = lax.dynamic_slice_in_dim(amino, dap_id * i_rows, i_rows).astype(F32)
    heads = [head_id ^ flip for flip in range(n_head)]
    row_keep = jnp.concatenate(
        [lax.dynamic_slice_in_dim(row_keep, h * mine, mine) for h in heads]
    )
    col_keep = lax.dynamic_slice_in_dim(amino, head_id * col_width, col_width).astype(F32)
    norm = jnp.maximum(
        total * row_keep[None, :, None] * col_keep.reshape(n_dap, 1, mine), 1.0
    )
    inverse = (1.0 / norm).reshape(n_dap * i_rows, mine)
    places = []
    for dz in STEPS:
        for dx in STEPS:
            for dy in range(ny):
                at_z, at_x, at_y = (zi + dz) % nz, (xi + dx) % nx, (yi + dy) % ny
                places.append((at_x * ny + at_y) * nz + at_z)
    place = jnp.stack([*places, *heads]).astype(jnp.int32)
    block, inverse, place = lax.optimization_barrier((block, inverse, place))
    rows, left, right = pl.pallas_call(
        attend_kernel,
        in_specs=[
            pl.BlockSpec(memory_space=pltpu.SMEM),
            whole(block.shape),
            *[whole(bundle.shape)] * n_head,
            whole((chans, 1)),
            whole((1, chans)),
            whole((1, chans)),
            whole((1, chans)),
            whole((1, chans)),
            whole((1, chans)),
            whole((seqs, 1)),
            whole((1, seqs)),
            whole((mine, chans, lanes)),
            whole((CO, chans)),
        ],
        out_specs=[
            whole((seqs * mine, chans)),
            whole((mine, CO, seqs)),
            whole((2, seqs // 2, lanes)),
        ],
        out_shape=[
            jax.ShapeDtypeStruct((seqs * mine, chans), BF16),
            jax.ShapeDtypeStruct((mine, CO, seqs), BF16),
            jax.ShapeDtypeStruct((2, seqs // 2, lanes), BF16),
        ],
        scratch_shapes=[
            pltpu.VMEM((chans, seqs), BF16),
            pltpu.VMEM((chans // DH, seqs, 128), BF16),
            pltpu.VMEM((chans, seqs), BF16),
            pltpu.VMEM((chans, seqs), F32),
            pltpu.VMEM((chans, seqs), BF16),
            pltpu.VMEM((chans // 128, seqs * mine, 128), F32),
            pltpu.VMEM((seqs, lanes), F32),
        ],
        compiler_params=pltpu.CompilerParams(
            vmem_limit_bytes=24 * 2**20
        ),
        cost_estimate=pl.CostEstimate(
            flops=16_000_000_000, bytes_accessed=4 * 2**20, transcendentals=9_000_000
        ),
        name="attend",
    )(
        own_amino,
        block,
        *bundles,
        shift,
        row(gain),
        row(bias),
        row(final_bias),
        row(gain2),
        row(bias2),
        keep.reshape(seqs, 1),
        keep.reshape(1, seqs),
        right_weight,
        left_weight,
    )

    swap = []
    for z in range(nz):
        for rest in range(nx * ny):
            for h in range(n_head):
                swap.append(
                    ((z * nx * ny + rest) * n_head + h, (h * nx * ny + rest) * n_head + z)
                )
    left = lax.ppermute(left, ("dap", "head"), swap)

    def shifted(value, axis, by):
        pairs = []
        for z in range(nz):
            for x in range(nx):
                for y in range(ny):
                    to = [z, x, y]
                    to[axis] = (to[axis] + by) % (nz, nx, ny)[axis]
                    pairs.append(((z * nx + x) * ny + y, (to[0] * nx + to[1]) * ny + to[2]))
        return lax.ppermute(value, "dap", pairs)

    other = shifted(right, 2, 1)

    def first_stage(value, axis):
        return [value] + [shifted(value, axis, -step) for step in STEPS[1:]]

    def second_stage(value, axis):
        from_left, from_right = shifted(value, axis, 1), shifted(value, axis, -1)
        return value, from_left, from_right

    colours = [jnp.stack([right[part], other[part]]) for part in range(2)]
    parts = first_stage(colours[0], 1) + first_stage(colours[1], 0)
    shape = (len(STEPS) * ny, *parts[0].shape[1:])
    mids = pl.pallas_call(
        join_kernel,
        in_specs=[pl.BlockSpec(memory_space=pltpu.VMEM)] * len(parts),
        out_specs=[pl.BlockSpec(memory_space=pltpu.VMEM)] * 2,
        out_shape=[jax.ShapeDtypeStruct(shape, BF16)] * 2,
        compiler_params=pltpu.CompilerParams(vmem_limit_bytes=4 * 2**20),
        cost_estimate=pl.CostEstimate(
            flops=2_000_000, bytes_accessed=2 * 2**20, transcendentals=0
        ),
        name="join",
    )(*parts)
    left_core = lax.ppermute(left, "head", swap_core)
    left_far = lax.ppermute(left, "head", [(h, h ^ 2) for h in range(n_head)])
    left_corner = lax.ppermute(left_far, "head", swap_core)
    z_pieces = second_stage(mids[0], 0)
    x_pieces = second_stage(mids[1], 1)
    half = len(STEPS) * ny // 2

    def forward(pieces, axis):
        return (*pieces, shifted(pieces[1][:half], axis, 1), shifted(pieces[2][half:], axis, -1))

    z_pieces = forward(z_pieces, 0)
    x_pieces = forward(x_pieces, 1)

    left = jnp.concatenate([left, left_core, left_far, left_corner], 0)
    left = jnp.swapaxes(left, 0, 1).reshape(CO * i_rows, seqs)

    back = lax.all_to_all(
        rows.reshape(n_dap * n_head, seqs * mine // (n_dap * n_head), chans),
        ("dap", "head"),
        split_axis=0,
        concat_axis=0,
        tiled=True,
    )
    own = own_seqs // n_head
    shared = (
        place,
        left,
        pair_bias.reshape(1, depth),
        inverse,
        pair_weight,
    )
    early = pl.pallas_call(
        early_kernel,
        in_specs=[
            pl.BlockSpec(memory_space=pltpu.SMEM),
            *[pl.BlockSpec(memory_space=pltpu.VMEM)] * 10,
        ],
        out_specs=pl.BlockSpec(memory_space=pltpu.VMEM),
        out_shape=jax.ShapeDtypeStruct((len(EARLY) * mine * i_rows, depth), F32),
        scratch_shapes=[
            pltpu.VMEM((len(EARLY) * i_rows, CO * lanes), BF16),
            pltpu.VMEM((CO * lanes, mine * depth), BF16),
        ],
        compiler_params=pltpu.CompilerParams(vmem_limit_bytes=18 * 2**20),
        cost_estimate=pl.CostEstimate(
            flops=3_000_000_000, bytes_accessed=6 * 2**20, transcendentals=0
        ),
        name="early",
    )(*shared, *z_pieces[:3], *x_pieces[:3])
    alignment = pl.pallas_call(
        arrange_kernel,
        in_specs=[pl.BlockSpec(memory_space=pltpu.VMEM)],
        out_specs=pl.BlockSpec(memory_space=pltpu.VMEM),
        out_shape=jax.ShapeDtypeStruct((own, residues, chans), BF16),
        compiler_params=pltpu.CompilerParams(vmem_limit_bytes=8 * 2**20),
        cost_estimate=pl.CostEstimate(
            flops=500_000_000, bytes_accessed=2 * 2**20, transcendentals=0
        ),
        name="arrange",
    )(back)
    part_specs = [
        pl.BlockSpec((ny, *z_pieces[0].shape[1:]), lambda _: (len(STEPS) - 1, 0, 0))
    ] * 3 + [pl.BlockSpec(memory_space=pltpu.VMEM)] * 2
    pair = pl.pallas_call(
        late_kernel,
        grid=(1,),
        in_specs=[
            pl.BlockSpec(memory_space=pltpu.SMEM),
            *[pl.BlockSpec(memory_space=pltpu.VMEM)] * 5,
            *part_specs,
            *part_specs,
        ],
        out_specs=pl.BlockSpec(memory_space=pltpu.VMEM),
        out_shape=jax.ShapeDtypeStruct((i_rows, col_width, depth), F32),
        scratch_shapes=[
            pltpu.VMEM((len(LATE) * i_rows, CO * lanes), BF16),
            pltpu.VMEM((CO * lanes, mine * depth), BF16),
            pltpu.VMEM((col_width * i_rows, depth), F32),
        ],
        compiler_params=pltpu.CompilerParams(vmem_limit_bytes=18 * 2**20),
        cost_estimate=pl.CostEstimate(
            flops=3_000_000_000, bytes_accessed=6 * 2**20, transcendentals=0
        ),
        name="late",
    )(*shared, early, *z_pieces, *x_pieces)
    return alignment, pair


def solution(mesh):
    return jax.shard_map(
        per_device,
        mesh=mesh,
        in_specs=(
            P("dap", None, None),
            P(),
            P(),
            P(),
            P(),
            P(None, None, "head"),
            P("head"),
            P("head", None),
            P(),
            P(),
            P(),
            P(),
            P(),
            P(),
        ),
        out_specs=(P(("dap", "head"), None, None), P("dap", "head", None)),
        check_vma=False,
    )
```
